512 devices in a mesh: dp: 64 (over x, y, core), rank: 8 (over z).
Axes of the slice: x: 4, y: 8, z: 8, core: 2. Of those that a mesh axis runs over, the one named last changes fastest.
Arguments:
- cloud_x: float32 [64, 131072], P(None, 'dp'), may hold values from -0.6 to 0.6
- cloud_y: float32 [64, 131072], P(None, 'dp'), may hold values from -0.6 to 0.6
- mass_x: float32 [131072], P('dp'), may hold values from 0.25 to 4
- mass_y: float32 [131072], P('dp'), may hold values from 0.25 to 4
- left_start: float32 [256, 131072], P('rank', 'dp'), may hold values from 0.25 to 204.8
- right_start: float32 [256, 131072], P('rank', 'dp'), may hold values from 0.25 to 204.8
- weight_start: float32 [256], P('rank'), may hold values from 0.25 to 4
Outputs:
- left_factor: float32 [256, 131072], P('rank', 'dp')
- right_factor: float32 [256, 131072], P('rank', 'dp')
- rank_weights: float32 [256], P('rank')
The draws below stay inside these ranges and needn't reach their ends.
All inputs are finite; a program needn't handle non-finite values.
Results may differ from the reference program's by a relative error of at most 0.0003.
Values sent between devices are 32-bit elements; how exact they have to be, the bound alone decides.
A program may use at most 64 MiB of HBM per device.

```python
import math
import jax
import jax.numpy as jnp
from jax import lax

DIM = 64
RANK = 256
INNER = 4
MIRROR = 3
N = 131072


def cluster_layout(key):
    centres = jax.random.normal(jax.random.fold_in(key, 7101), (DIM, RANK), jnp.float32) * jnp.sqrt(0.6 / DIM)
    shifted = centres + jax.random.normal(jax.random.fold_in(key, 7102), (DIM, RANK), jnp.float32) * jnp.sqrt(0.2 / DIM)
    member_x = jax.random.randint(jax.random.fold_in(key, 7103), (N,), 0, RANK).astype(jnp.int32)
    member_y = jax.random.randint(jax.random.fold_in(key, 7104), (N,), 0, RANK).astype(jnp.int32)
    return (centres, shifted, member_x, member_y)


def cloud_points(key, centres, member, salt):
    base = jnp.take(centres, member, axis=1)
    noise_key = jax.random.fold_in(key, salt)
    noise = jax.random.normal(noise_key, (DIM, N), jnp.float32) * jnp.sqrt(0.5 / DIM)
    return jnp.clip(base + noise, -0.6, 0.6)


def factor_start(key, member, salt):
    rest = jnp.exp(jax.random.uniform(jax.random.fold_in(key, salt), (RANK, N), jnp.float32, jnp.log(0.25), jnp.log(4.0)))
    own = RANK * jnp.exp(jax.random.uniform(jax.random.fold_in(key, salt + 1), (RANK, N), jnp.float32, jnp.log(0.25), jnp.log(0.8)))
    match = jnp.arange(RANK, dtype=jnp.int32)[:, None] == member[None, :]
    return jnp.where(match, own, rest)


def draw_cloud_x(key, part):
    centres, shifted, member_x, member_y = cluster_layout(key)
    return cloud_points(key, centres, member_x, 7201)


def draw_cloud_y(key, part):
    centres, shifted, member_x, member_y = cluster_layout(key)
    return cloud_points(key, shifted, member_y, 7301)


def draw_left_start(key, part):
    centres, shifted, member_x, member_y = cluster_layout(key)
    return factor_start(key, member_x, 7401)


def draw_right_start(key, part):
    centres, shifted, member_x, member_y = cluster_layout(key)
    return factor_start(key, member_y, 7501)


def level_of(key, extent, shards, least, largest):
    def one(dim, shards_of):
        steps = jax.random.uniform(jax.random.fold_in(jax.random.fold_in(key, 6), dim), (shards_of,), jnp.float32, least / len(shards), largest / len(shards))
        return jnp.repeat(jnp.exp(steps), extent[dim] // shards_of).reshape((-1,) + (1,) * (len(extent) - dim - 1))

    gain = one(*shards[0])
    for cut in shards[1:]:
        gain = gain * one(*cut)
    return gain


def setup_inputs(seed: int = 0) -> dict:
    key_of = jax.random.split(jax.random.key(seed), 8)
    cloud_x = draw_cloud_x(jax.random.fold_in(key_of[7], 71), 0)
    cloud_y = draw_cloud_y(jax.random.fold_in(key_of[7], 71), 0)
    mass_x = jnp.clip(jnp.exp(math.log(4.0) - 2.7725887 * jax.random.uniform(key_of[2], (N,), jnp.float32) ** level_of(key_of[2], (N,), ((0, 64),), -0.2, 0.2)), 0.25, 4.0)
    mass_y = jnp.clip(jnp.exp(math.log(4.0) - 2.7725887 * jax.random.uniform(key_of[3], (N,), jnp.float32) ** level_of(key_of[3], (N,), ((0, 64),), -0.2, 0.2)), 0.25, 4.0)
    left_start = draw_left_start(jax.random.fold_in(key_of[7], 71), 0)
    right_start = draw_right_start(jax.random.fold_in(key_of[7], 71), 0)
    weight_start = jnp.clip(jnp.exp(math.log(4.0) - 2.7725887 * jax.random.uniform(key_of[6], (RANK,), jnp.float32) ** level_of(key_of[6], (RANK,), ((0, 8),), -0.2, 0.2)), 0.25, 4.0)
    return dict(cloud_x=cloud_x, cloud_y=cloud_y, mass_x=mass_x, mass_y=mass_y, left_start=left_start, right_start=right_start, weight_start=weight_start)


exact_mode = lax.Precision.HIGHEST
step_size = 2.0


def project(kernel_left, kernel_right, kernel_weight, left_mass, right_mass):
    scale_left = jnp.ones((RANK,), jnp.float32)
    scale_right = jnp.ones((RANK,), jnp.float32)
    for repeat in range(INNER):
        point_left = left_mass / jnp.dot(scale_left, kernel_left, precision=exact_mode)
        point_right = right_mass / jnp.dot(scale_right, kernel_right, precision=exact_mode)
        column_left = jnp.dot(kernel_left, point_left, precision=exact_mode)
        column_right = jnp.dot(kernel_right, point_right, precision=exact_mode)
        weights = jnp.cbrt(kernel_weight * scale_left * column_left * scale_right * column_right)
        scale_left = weights / column_left
        scale_right = weights / column_right
    left = point_left[None, :] * kernel_left * scale_left[:, None]
    right = point_right[None, :] * kernel_right * scale_right[:, None]
    return left, right, weights


def moments(cloud, factor):
    product = jnp.dot(cloud, factor.T, precision=exact_mode)
    square = jnp.dot(factor, jnp.sum(cloud * cloud, axis=0), precision=exact_mode)
    column = jnp.sum(factor, axis=1)
    return product, square, column


def reference(cloud_x, cloud_y, mass_x, mass_y, left_start, right_start, weight_start):
    left_mass = mass_x * (N / jnp.sum(mass_x))
    right_mass = mass_y * (N / jnp.sum(mass_y))
    left, right, weights = project(left_start, right_start, weight_start, left_mass, right_mass)
    for outer in range(MIRROR):
        prod_x, square_x, sums_q = moments(cloud_x, left)
        prod_y, square_y, sums_r = moments(cloud_y, right)
        grad_q = square_y / weights
        grad_r = square_x / weights
        grad_g = -(square_x * sums_r + sums_q * square_y - 2.0 * jnp.sum(prod_x * prod_y, axis=0)) / (weights * weights)
        mean_q = jnp.sum(grad_q) / RANK
        mean_r = jnp.sum(grad_r) / RANK
        mean_g = jnp.sum(grad_g) / RANK
        field_q = (grad_q - mean_q)[:, None] - 2.0 * jnp.dot(prod_y.T, cloud_x, precision=exact_mode) / weights[:, None]
        field_r = (grad_r - mean_r)[:, None] - 2.0 * jnp.dot(prod_x.T, cloud_y, precision=exact_mode) / weights[:, None]
        kernel_left = left * jnp.exp(-step_size * field_q)
        kernel_right = right * jnp.exp(-step_size * field_r)
        kernel_weight = weights * jnp.exp(-step_size * (grad_g - mean_g))
        left, right, weights = project(kernel_left, kernel_right, kernel_weight, left_mass, right_mass)
    return RANK * left, RANK * right, (RANK / N) * weights
```

```python
import functools

import jax
import jax.numpy as jnp
from jax import lax
from jax.experimental import pallas as pl
from jax.experimental.pallas import tpu as pltpu
from jax.sharding import PartitionSpec as P

RANK = 256
INNER = 4
MIRROR = 3
STEP = 2.0
MESH = pl.DeviceIdType.MESH
EXACT = lax.Precision.HIGHEST

NX, NY, NC, NZ = 4, 8, 2, 8
NDP = NX * NY * NC


def far_first(n):
    return sorted(range(n), key=lambda d: -min(d, n - d))


DP_OFFSETS = sorted(
    [(dx, dy, dc) for dx in range(NX) for dy in range(NY) for dc in range(NC) if (dx, dy, dc) != (0, 0, 0)],
    key=lambda o: -(min(o[0], NX - o[0]) + min(o[1], NY - o[1])),
)
XC_OFFSETS = [o for o in DP_OFFSETS if o[1] == 0]
Y_OFFSETS = [o for o in DP_OFFSETS if o[0] == 0 and o[2] == 0]
Z_OFFSETS = [d for d in far_first(NZ) if d]


def cube_root(x):
    y = jnp.exp2(jnp.log2(x) * (1.0 / 3.0))
    y = y - (y - x / (y * y)) * (1.0 / 3.0)
    return jnp.where(x > 0.0, y, 0.0)


def kernel(
    total_count,
    x_ref, y_ref, mx_ref, my_ref, left_ref, right_ref, w_ref,
    lo_ref, ro_ref, wo_ref,
    k_s, uk_s, xy_s, a_s, n2_s, u_s, vb_s, v_s, k3_s, sc_s, s_s, g_s, c_s,
    zbuf, cbuf, xbuf, ybuf, mbuf,
    zsend, zrecv, csend, crecv, xsend, xrecv, ysend, yrecv, msend, mrecv,
):
    dp = lax.axis_index("dp")
    z = lax.axis_index("rank")
    core = lax.rem(dp, NC)
    yy = lax.rem(lax.div(dp, NC), NY)
    xx = lax.div(dp, NC * NY)
    xc = xx * NC + core
    tiles = left_ref.shape[1] // 128

    def dp_target(o):
        tx = lax.rem(xx + o[0], NX)
        ty = lax.rem(yy + o[1], NY)
        tc = lax.rem(core + o[2], NC)
        return ((tx * NY + ty) * NC + tc, z)

    def z_target(d):
        return (dp, lax.rem(z + d, NZ))

    barrier = pltpu.get_barrier_semaphore()
    for d in Z_OFFSETS:
        pl.semaphore_signal(barrier, inc=1, device_id=z_target(d), device_id_type=MESH)
    for o in DP_OFFSETS:
        pl.semaphore_signal(barrier, inc=1, device_id=dp_target(o), device_id_type=MESH)

    def send(slot, targets, ssem, rsem):
        for t in targets:
            pltpu.make_async_remote_copy(
                src_ref=slot, dst_ref=slot, send_sem=ssem, recv_sem=rsem, device_id=t, device_id_type=MESH
            ).start()

    def wait(some, ssem, rsem):
        pltpu.make_async_copy(some, some, rsem).wait()
        pltpu.make_async_copy(some, some, ssem).wait()

    k_s[0:32, :] = left_ref[...]
    k_s[32:64, :] = right_ref[...]
    xy_s[0:64, :] = x_ref[...]
    xy_s[64:128, :] = y_ref[...]
    a_s[0:tiles, :] = mx_ref[...]
    a_s[tiles:2 * tiles, :] = my_ref[...]
    for t in range(tiles):
        bx = xy_s[0:64, t * 128:(t + 1) * 128]
        by = xy_s[64:128, t * 128:(t + 1) * 128]
        n2_s[t:t + 1, :] = jnp.sum(bx * bx, axis=0, keepdims=True)
        n2_s[tiles + t:tiles + t + 1, :] = jnp.sum(by * by, axis=0, keepdims=True)
    k3_s[...] = w_ref[...]
    sc_s[...] = jnp.ones((1, 128), jnp.float32)
    lane = lax.broadcasted_iota(jnp.int32, (1, 128), 1)
    pl.semaphore_wait(barrier, len(Z_OFFSETS) + len(DP_OFFSETS))

    def spread(vec):
        return jnp.broadcast_to(vec, (128, 128)).T

    def gather_rows(rows):
        return jnp.sum(rows.T, axis=0, keepdims=True)

    def doubled(c):
        return jnp.where(lane < 64, c, pltpu.roll(c, 64, 1))

    def row_sums(par):
        for t in range(tiles):
            b = k_s[:, t * 128:(t + 1) * 128] * vb_s[...]
            zbuf[par, z, t:t + 1, :] = jnp.sum(b[0:32], axis=0, keepdims=True)
            zbuf[par, z, tiles + t:tiles + t + 1, :] = jnp.sum(b[32:64], axis=0, keepdims=True)
        send(zbuf.at[par, z], [z_target(d) for d in Z_OFFSETS], zsend.at[par], zrecv.at[par])
        wait(zbuf.at[par, 0:NZ - 1], zsend.at[par], zrecv.at[par])
        total = zbuf[par, 0]
        for i in range(1, NZ):
            total = total + zbuf[par, i]
        u_s[...] = a_s[...] / total

    def column_parts(weights):
        accs = [jnp.zeros((64, 128), jnp.float32) for _ in weights]
        for t in range(tiles):
            b = k_s[:, t * 128:(t + 1) * 128]
            for j, w in enumerate(weights):
                wl = jnp.broadcast_to(w[t:t + 1, :], (32, 128))
                wr = jnp.broadcast_to(w[tiles + t:tiles + t + 1, :], (32, 128))
                accs[j] = accs[j] + b * jnp.concatenate([wl, wr], axis=0)
        return accs

    def start_columns(par, low, high):
        cbuf[par, dp] = gather_rows(jnp.concatenate([low, high], axis=0))
        send(cbuf.at[par, dp], [dp_target(o) for o in DP_OFFSETS], csend.at[par], crecv.at[par])

    def end_columns(par):
        wait(cbuf.at[par, 0:NDP - 1], csend.at[par], crecv.at[par])
        parts = [cbuf[par, i] for i in range(4)]
        for i in range(4, NDP):
            parts[i % 4] = parts[i % 4] + cbuf[par, i]
        return (parts[0] + parts[1]) + (parts[2] + parts[3])

    def rescale(c):
        v = v_s[...]
        p = v * c
        g = cube_root(k3_s[...] * p * pltpu.roll(p, 32, 1))
        v = g / c
        v_s[...] = v
        g_s[...] = g
        return v

    def plain_step(step):
        par = lax.rem(step, 2)
        row_sums(par)
        (low,) = column_parts([u_s])
        half = tiles
        ax = jnp.sum(a_s[0:half, :], axis=0, keepdims=True)
        ay = jnp.sum(a_s[half:2 * half, :], axis=0, keepdims=True)
        high = jnp.concatenate([jnp.broadcast_to(ax, (32, 128)), jnp.broadcast_to(ay, (32, 128))], axis=0)
        start_columns(par, low, high)
        c = end_columns(par)
        mass = jnp.where(lane >= 64, c, pltpu.roll(c, 64, 1))
        scale = total_count / mass
        sc_s[...] = scale
        v = rescale(doubled(c) * scale)
        vb_s[...] = spread(v)[0:64]

    def last_step(step, moments):
        par = lax.rem(step, 2)
        row_sums(par)
        if moments:
            for t in range(tiles):
                n2_s[2 * tiles + t:2 * tiles + t + 1, :] = u_s[t:t + 1, :] * n2_s[t:t + 1, :]
                n2_s[3 * tiles + t:3 * tiles + t + 1, :] = u_s[tiles + t:tiles + t + 1, :] * n2_s[tiles + t:tiles + t + 1, :]
            low, high = column_parts([u_s, n2_s.at[2 * tiles:4 * tiles]])
        else:
            (low,) = column_parts([u_s])
            high = low
        start_columns(par, low, high)
        for t in range(tiles):
            cols = slice(t * 128, (t + 1) * 128)
            uk_s[0:32, cols] = k_s[0:32, cols] * jnp.broadcast_to(u_s[t:t + 1, :], (32, 128))
            uk_s[32:64, cols] = k_s[32:64, cols] * jnp.broadcast_to(u_s[tiles + t:tiles + t + 1, :], (32, 128))
        if moments:
            both = lax.dot_general(
                uk_s[...], xy_s[...], (((1,), (1,)), ((), ())),
                precision=EXACT, preferred_element_type=jnp.float32,
            )
            xbuf[xc] = jnp.where(lane < 64, both[0:32], both[32:64])
            send(xbuf.at[xc], [dp_target(o) for o in XC_OFFSETS], xsend, xrecv)
        c = end_columns(par)
        scale = sc_s[...]
        cn = doubled(c) * scale
        v = rescale(cn)
        return c, cn, v, v * scale

    def projection(base, moments):
        v_s[...] = jnp.ones((1, 128), jnp.float32)
        vb_s[...] = jnp.ones((64, 128), jnp.float32)

        def body(t, carry):
            plain_step(base + t)
            return carry

        lax.fori_loop(0, INNER - 1, body, 0)
        return last_step(base + (INNER - 1), moments)

    def mirror(outer, carry):
        c, cn, v, veff = projection(outer * INNER, True)
        g = g_s[...]
        wait(xbuf.at[0:NX * NC - 1], xsend, xrecv)
        m = xbuf[0]
        for i in range(1, NX * NC):
            m = m + xbuf[i]
        ybuf[yy] = m
        send(ybuf.at[yy], [dp_target(o) for o in Y_OFFSETS], ysend, yrecv)
        sq = jnp.where(lane < 64, pltpu.roll(c, 64, 1), c) * veff
        qs = cn * v
        cross = sq * pltpu.roll(qs, 32, 1)
        cross = cross + pltpu.roll(cross, 32, 1)
        hh = pltpu.roll(sq, 32, 1) / g
        swapped = pltpu.roll(veff, 32, 1)
        wait(ybuf.at[0:NY - 1], ysend, yrecv)
        m = ybuf[0]
        for i in range(1, NY):
            m = m + ybuf[i]
        turned = pltpu.roll(m, 64, 1)
        prod = m * turned
        dots = jnp.sum(jnp.concatenate([prod] * 4, axis=0).T[0:64], axis=0, keepdims=True)
        gg = -(cross - 2.0 * dots * veff * swapped) / (g * g)
        mbuf[z] = jnp.where(lane < 64, hh, jnp.where(lane < 96, gg, 0.0))
        send(mbuf.at[z], [z_target(d) for d in Z_OFFSETS], msend, mrecv)
        factor = spread(swapped * (2.0 * STEP) / g)[0:64]
        wide = lax.broadcasted_iota(jnp.int32, (32, 128), 1)
        w = jnp.concatenate([jnp.where(wide < 64, turned, 0.0), jnp.where(wide < 64, 0.0, turned)], axis=0) * factor
        qv = spread(veff)[0:64]
        wait(mbuf.at[0:NZ - 1], msend, mrecv)
        s = mbuf[0]
        for i in range(1, NZ):
            s = s + mbuf[i]
        mq = jnp.sum(jnp.where(lane < 32, s, 0.0), axis=1, keepdims=True) / RANK
        mr = jnp.sum(jnp.where((lane >= 32) & (lane < 64), s, 0.0), axis=1, keepdims=True) / RANK
        mg = jnp.sum(jnp.where((lane >= 64) & (lane < 96), s, 0.0), axis=1, keepdims=True) / RANK
        mean = jnp.where(lax.rem(lane, 64) < 32, mq, mr)
        shift = spread((hh - mean) * (-STEP))[0:64]
        k3_s[...] = g * jnp.exp(-STEP * (gg - mg))
        for t in range(tiles // 2):
            cols = slice(t * 256, (t + 1) * 256)
            f = lax.dot_general(
                w, xy_s[:, cols], (((1,), (0,)), ((), ())),
                precision=EXACT, preferred_element_type=jnp.float32,
            )
            sh = jnp.concatenate([shift, shift], axis=1)
            q2 = jnp.concatenate([qv, qv], axis=1)
            k_s[:, cols] = uk_s[:, cols] * q2 * jnp.exp(f + sh)
        return carry

    lax.fori_loop(0, MIRROR, mirror, 0)
    _, _, v, veff = projection(MIRROR * INNER, False)
    qv = spread(veff * RANK)[0:64]
    for t in range(tiles):
        cols = slice(t * 128, (t + 1) * 128)
        out = uk_s[:, cols] * qv
        lo_ref[:, cols] = out[0:32]
        ro_ref[:, cols] = out[32:64]
    wo_ref[...] = g_s[...] * (RANK / total_count)


def shards(cloud_x, cloud_y, mass_x, mass_y, left_start, right_start, weight_start):
    ranks, points = left_start.shape
    total_count = float(points * lax.axis_size("dp"))
    tiles = points // 128
    f32 = jnp.float32
    dma = pltpu.SemaphoreType.DMA
    left, right, weights = pl.pallas_call(
        functools.partial(kernel, total_count),
        name="sinkhorn",
        out_shape=(
            jax.ShapeDtypeStruct((ranks, points), f32),
            jax.ShapeDtypeStruct((ranks, points), f32),
            jax.ShapeDtypeStruct((1, 128), f32),
        ),
        in_specs=[pl.BlockSpec(memory_space=pltpu.VMEM)] * 7,
        out_specs=[pl.BlockSpec(memory_space=pltpu.VMEM)] * 3,
        scratch_shapes=[
            pltpu.VMEM((2 * ranks, points), f32),
            pltpu.VMEM((2 * ranks, points), f32),
            pltpu.VMEM((128, points), f32),
            pltpu.VMEM((2 * tiles, 128), f32),
            pltpu.VMEM((4 * tiles, 128), f32),
            pltpu.VMEM((2 * tiles, 128), f32),
            pltpu.VMEM((64, 128), f32),
            pltpu.VMEM((1, 128), f32),
            pltpu.VMEM((1, 128), f32),
            pltpu.VMEM((1, 128), f32),
            pltpu.VMEM((1, 128), f32),
            pltpu.VMEM((1, 128), f32),
            pltpu.VMEM((1, 128), f32),
            pltpu.VMEM((2, NZ, 2 * tiles, 128), f32),
            pltpu.VMEM((2, NDP, 1, 128), f32),
            pltpu.VMEM((NX * NC, 32, 128), f32),
            pltpu.VMEM((NY, 32, 128), f32),
            pltpu.VMEM((NZ, 1, 128), f32),
            dma((2,)), dma((2,)), dma((2,)), dma((2,)),
            dma, dma, dma, dma, dma, dma,
        ],
        compiler_params=pltpu.CompilerParams(collective_id=0, has_side_effects=True),
    )(
        cloud_x, cloud_y, mass_x.reshape(tiles, 128), mass_y.reshape(tiles, 128),
        left_start, right_start, jnp.tile(weight_start, 4)[None],
    )
    return left, right, weights[0, :ranks]


def solution(mesh):
    in_specs = (
        P(None, "dp"),
        P(None, "dp"),
        P("dp"),
        P("dp"),
        P("rank", "dp"),
        P("rank", "dp"),
        P("rank"),
    )
    out_specs = (P("rank", "dp"), P("rank", "dp"), P("rank"))
    return jax.shard_map(shards, mesh=mesh, in_specs=in_specs, out_specs=out_specs, check_vma=False)
```

```python
import functools

import jax
import jax.numpy as jnp
from jax import lax
from jax.experimental import pallas as pl
from jax.experimental.pallas import tpu as pltpu
from jax.sharding import PartitionSpec as P

RANK = 256
INNER = 4
MIRROR = 3
STEP = 2.0
MESH = pl.DeviceIdType.MESH
EXACT = lax.Precision.HIGHEST
LOG2E = 1.4426950408889634

NX, NY, NC, NZ = 4, 8, 2, 8
NDP = NX * NY * NC


def far_first(n):
    return sorted(range(n), key=lambda d: -min(d, n - d))


DP_OFFSETS = sorted(
    [(dx, dy, dc) for dx in range(NX) for dy in range(NY) for dc in range(NC) if (dx, dy, dc) != (0, 0, 0)],
    key=lambda o: -(min(o[0], NX - o[0]) + min(o[1], NY - o[1])),
)
XC_OFFSETS = [o for o in DP_OFFSETS if o[1] == 0]
Y_OFFSETS = [o for o in DP_OFFSETS if o[0] == 0 and o[2] == 0]
Z_OFFSETS = [d for d in far_first(NZ) if d]


def cube_root(x):
    y = jnp.exp2(jnp.log2(x) * (1.0 / 3.0))
    y = y - (y - x / (y * y)) * (1.0 / 3.0)
    return jnp.where(x > 0.0, y, 0.0)


def split(x):
    high = x.astype(jnp.bfloat16)
    return high, (x - high.astype(jnp.float32)).astype(jnp.bfloat16)


def kernel(
    total_count,
    x_ref, y_ref, mx_ref, my_ref, left_ref, right_ref, w_ref,
    lo_ref, ro_ref, wo_ref,
    k_s, c_s, uk_s, xy_s, x4_s, w4_s, a_s, n2_s, u_s, vb_s, fb_s, sb_s,
    v1_s, k1_s, sc_s, v_s, k3_s, g_s, veff_s, qs_s,
    zbuf, cbuf, dbuf, xbuf, ybuf, mbuf,
    zsend, zrecv, csend, crecv, dsend, drecv, xsend, xrecv, ysend, yrecv, msend, mrecv, asend, arecv,
):
    dp = lax.axis_index("dp")
    z = lax.axis_index("rank")
    core = lax.rem(dp, NC)
    yy = lax.rem(lax.div(dp, NC), NY)
    xx = lax.div(dp, NC * NY)
    xc = xx * NC + core
    tiles = left_ref.shape[1] // 128
    half = left_ref.shape[0]

    def dp_target(o):
        tx = lax.rem(xx + o[0], NX)
        ty = lax.rem(yy + o[1], NY)
        tc = lax.rem(core + o[2], NC)
        return ((tx * NY + ty) * NC + tc, z)

    def z_target(d):
        return (dp, lax.rem(z + d, NZ))

    barrier = pltpu.get_barrier_semaphore()
    for d in Z_OFFSETS:
        pl.semaphore_signal(barrier, inc=1, device_id=z_target(d), device_id_type=MESH)
    for o in DP_OFFSETS:
        pl.semaphore_signal(barrier, inc=1, device_id=dp_target(o), device_id_type=MESH)

    def send(slot, targets, ssem, rsem):
        for t in targets:
            pltpu.make_async_remote_copy(
                src_ref=slot, dst_ref=slot, send_sem=ssem, recv_sem=rsem, device_id=t, device_id_type=MESH
            ).start()

    def wait(some, ssem, rsem):
        pltpu.make_async_copy(some, some, rsem).wait()
        pltpu.make_async_copy(some, some, ssem).wait()

    def tile(t):
        return slice(t * 128, (t + 1) * 128)

    k_s[z, 0:half, :] = left_ref[...]
    k_s[z, half:2 * half, :] = right_ref[...]
    xy_s[0:64, :] = x_ref[...]
    xy_s[64:128, :] = y_ref[...]
    a_s[0:tiles, :] = mx_ref[...]
    a_s[tiles:2 * tiles, :] = my_ref[...]
    lane = lax.broadcasted_iota(jnp.int32, (1, 128), 1)
    wide = lax.broadcasted_iota(jnp.int32, (4, 128), 1)
    pl.semaphore_wait(barrier, len(Z_OFFSETS) + len(DP_OFFSETS))

    def spread(vec):
        return jnp.broadcast_to(vec, (128, 128)).T

    def spread_all(dst, packed):
        for r in range(4):
            s = spread(packed[r:r + 1])
            dst[r] = s[0:64]
            dst[r + 4] = s[64:128]

    def gather_rows(rows):
        return jnp.sum(rows.T, axis=0, keepdims=True)

    def swap(p):
        return jnp.where(lax.rem(lax.broadcasted_iota(jnp.int32, p.shape, 1), 64) < 32, pltpu.roll(p, 96, 1), pltpu.roll(p, 32, 1))

    def doubled(c):
        return jnp.where(lane < 64, c, pltpu.roll(c, 64, 1))

    def packed(rows):
        return jnp.concatenate([jnp.where(lane < 64, rows[r], rows[r + 4]) for r in range(4)], axis=0)

    def ring(hop, go):
        for way, sign in ((0, 1), (1, -1)):
            block = lax.rem(z - sign * hop + NZ, NZ)
            part = k_s.at[block]
            if hop == NZ // 2 - 1:
                part = k_s.at[block, half * way:half * (way + 1)]
            copy = pltpu.make_async_remote_copy(
                src_ref=part, dst_ref=part, send_sem=asend.at[hop, way], recv_sem=arecv.at[hop, way],
                device_id=(dp, lax.rem(z + sign + NZ, NZ)), device_id_type=MESH,
            )
            if go:
                copy.start()
            else:
                copy.wait_recv()
                copy.wait_send()

    def ring_step(step):
        for hop in range(NZ // 2):
            @pl.when(step == hop)
            def _():
                if hop:
                    ring(hop - 1, False)
                ring(hop, True)

    def row_sums(step):
        par = lax.rem(step, 2)
        for t in range(tiles):
            b = k_s[z, :, tile(t)] * vb_s[0]
            zbuf[par, z, t:t + 1, :] = jnp.sum(b[0:half], axis=0, keepdims=True)
            zbuf[par, z, tiles + t:tiles + t + 1, :] = jnp.sum(b[half:2 * half], axis=0, keepdims=True)
        send(zbuf.at[par, z], [z_target(d) for d in Z_OFFSETS], zsend.at[par], zrecv.at[par])
        ring_step(step)

        @pl.when(step == 0)
        def _():
            prepare()

        wait(zbuf.at[par, 0:NZ - 1], zsend.at[par], zrecv.at[par])
        total = zbuf[par, 0]
        for i in range(1, NZ):
            total = total + zbuf[par, i]
        u_s[...] = a_s[...] / total

    def prepare():
        for t in range(tiles):
            bx = xy_s[0:64, tile(t)]
            by = xy_s[64:128, tile(t)]
            n2_s[t:t + 1, :] = jnp.sum(bx * bx, axis=0, keepdims=True)
            n2_s[tiles + t:tiles + t + 1, :] = jnp.sum(by * by, axis=0, keepdims=True)
            for i, b in enumerate((bx, by)):
                high, low = split(b)
                both = jnp.concatenate([high, low], axis=0)
                x4_s[i, 0:128, tile(t)] = both
                x4_s[i, 128:256, tile(t)] = both

    def own_parts(w):
        acc = jnp.zeros((64, 128), jnp.float32)
        for t in range(tiles):
            wl = jnp.broadcast_to(w[t:t + 1, :], (half, 128))
            wr = jnp.broadcast_to(w[tiles + t:tiles + t + 1, :], (half, 128))
            acc = acc + k_s[z, :, tile(t)] * jnp.concatenate([wl, wr], axis=0)
        return acc

    def exchange_columns(par):
        send(cbuf.at[par, dp], [dp_target(o) for o in DP_OFFSETS], csend.at[par], crecv.at[par])

    def summed(buf, par):
        parts = [buf[par, i] for i in range(4)]
        for i in range(4, NDP):
            parts[i % 4] = parts[i % 4] + buf[par, i]
        return (parts[0] + parts[1]) + (parts[2] + parts[3])

    def rescale(c, v_ref, k_ref):
        v = v_ref[...]
        p = v * c
        g = cube_root(k_ref[...] * p * swap(p))
        v = g / c
        v_ref[...] = v
        return g, v

    def first_step(step, carry):
        par = lax.rem(step, 2)
        row_sums(step)
        low = own_parts(u_s)
        ax = jnp.sum(a_s[0:tiles, :], axis=0, keepdims=True)
        ay = jnp.sum(a_s[tiles:2 * tiles, :], axis=0, keepdims=True)
        high = jnp.concatenate([jnp.broadcast_to(ax, (32, 128)), jnp.broadcast_to(ay, (32, 128))], axis=0)
        cbuf[par, dp] = gather_rows(jnp.concatenate([low, high], axis=0))
        exchange_columns(par)
        wait(cbuf.at[par, 0:NDP - 1], csend.at[par], crecv.at[par])
        c = summed(cbuf, par)
        scale = total_count / jnp.where(lane >= 64, c, pltpu.roll(c, 64, 1))
        sc_s[...] = scale
        g, v = rescale(doubled(c) * scale, v1_s, k1_s)
        vb_s[0] = spread(v)[0:64]
        return carry

    def start_moments():
        for t in range(tiles):
            uk_s[0:half, tile(t)] = k_s[z, 0:half, tile(t)] * jnp.broadcast_to(u_s[t:t + 1, :], (half, 128))
            uk_s[half:2 * half, tile(t)] = k_s[z, half:2 * half, tile(t)] * jnp.broadcast_to(u_s[tiles + t:tiles + t + 1, :], (half, 128))
        acc = jnp.zeros((64, 128), jnp.float32)
        for t in range(tiles):
            nl = jnp.broadcast_to(n2_s[t:t + 1, :], (half, 128))
            nr = jnp.broadcast_to(n2_s[tiles + t:tiles + t + 1, :], (half, 128))
            acc = acc + uk_s[:, tile(t)] * jnp.concatenate([nl, nr], axis=0)
        both = lax.dot_general(
            uk_s[...], xy_s[...], (((1,), (1,)), ((), ())), precision=EXACT, preferred_element_type=jnp.float32
        )
        xbuf[xc, 0:32] = jnp.where(lane < 64, both[0:half], both[half:2 * half])
        xbuf[xc, 32:40] = jnp.broadcast_to(gather_rows(jnp.concatenate([acc, acc], axis=0)), (8, 128))
        send(xbuf.at[xc], [dp_target(o) for o in XC_OFFSETS], xsend, xrecv)

    def middle_moments():
        wait(xbuf.at[0:NX * NC - 1], xsend, xrecv)
        m = xbuf[0]
        for i in range(1, NX * NC):
            m = m + xbuf[i]
        ybuf[yy] = m
        send(ybuf.at[yy], [dp_target(o) for o in Y_OFFSETS], ysend, yrecv)

    def end_moments(par, rows):
        wait(ybuf.at[0:NY - 1], ysend, yrecv)
        m = ybuf[0]
        for i in range(1, NY):
            m = m + ybuf[i]
        mbuf[par, z] = m
        for i, row in enumerate(rows):
            mbuf[par, z, 33 + i:34 + i] = row
        send(mbuf.at[par, z], [z_target(d) for d in Z_OFFSETS], msend.at[par], mrecv.at[par])

    v1_s[...] = jnp.ones((1, 128), jnp.float32)
    k1_s[...] = w_ref[...]
    vb_s[0] = jnp.ones((64, 128), jnp.float32)
    lax.fori_loop(0, INNER - 1, first_step, 0)
    par = (INNER - 1) % 2
    row_sums(INNER - 1)
    start_moments()
    low = own_parts(u_s)
    cbuf[par, dp] = gather_rows(jnp.concatenate([low, low], axis=0))
    exchange_columns(par)
    middle_moments()
    wait(cbuf.at[par, 0:NDP - 1], csend.at[par], crecv.at[par])
    c1 = summed(cbuf, par) * sc_s[...]
    g1, v1 = rescale(c1, v1_s, k1_s)
    end_moments(0, (g1, v1 * sc_s[...], c1 * v1))
    ring(NZ // 2 - 1, False)
    wait(mbuf.at[0, 0:NZ - 1], msend.at[0], mrecv.at[0])
    g_s[...] = packed([mbuf[0, b, 33:34] for b in range(NZ)])
    veff_s[...] = packed([mbuf[0, b, 34:35] for b in range(NZ)])
    qs_s[...] = packed([mbuf[0, b, 35:36] for b in range(NZ)])

    def u_of_rows():
        for side in range(2):
            def body(b, accs):
                accs = list(accs)
                for j in range(half // 8):
                    rows = slice(side * half + 8 * j, side * half + 8 * j + 8)
                    v = vb_s[b, rows]
                    for t in range(tiles):
                        accs[t] = accs[t] + k_s[b, rows, tile(t)] * v
                return tuple(accs)

            accs = lax.fori_loop(0, NZ, body, tuple(jnp.zeros((8, 128), jnp.float32) for _ in range(tiles)))
            for t in range(tiles):
                i = side * tiles + t
                u_s[i:i + 1, :] = a_s[i:i + 1, :] / jnp.sum(accs[t], axis=0, keepdims=True)

    def start_columns(par):
        for side in range(2):
            us = [jnp.broadcast_to(u_s[side * tiles + t:side * tiles + t + 1, :], (8, 128)) for t in range(tiles)]

            def body(b, carry):
                for j in range(half // 8):
                    rows = slice(side * half + 8 * j, side * half + 8 * j + 8)
                    acc = [k_s[b, rows, tile(t)] * us[t] for t in range(tiles)]
                    while len(acc) > 1:
                        acc = [p + q for p, q in zip(acc[::2], acc[1::2])]
                    c_s[b, rows] = acc[0]
                return carry

            lax.fori_loop(0, NZ, body, 0)
        dbuf[par, dp] = jnp.concatenate(
            [gather_rows(jnp.concatenate([c_s[r], c_s[r + 4]], axis=0)) for r in range(4)], axis=0
        )
        send(dbuf.at[par, dp], [dp_target(o) for o in DP_OFFSETS], dsend.at[par], drecv.at[par])

    def end_columns(par):
        wait(dbuf.at[par, 0:NDP - 1], dsend.at[par], drecv.at[par])
        c = summed(dbuf, par) * sc_s[...]
        g, v = rescale(c, v_s, k3_s)
        return c, g, v

    def plain_step(step):
        par = lax.rem(step, 2)
        u_of_rows()
        start_columns(par)
        _, _, v = end_columns(par)
        spread_all(vb_s, v)

    def mirror(outer, carry):
        mpar = lax.rem(outer, 2)
        g = g_s[...]
        veff = veff_s[...]
        qs = qs_s[...]
        sq = packed([mbuf[mpar, b, 32:33] for b in range(NZ)]) * veff
        cross = sq * swap(qs)
        cross = cross + swap(cross)
        other = swap(veff)
        dots = []
        for r in range(4):
            prods = [mbuf[mpar, b, 0:32] * pltpu.roll(mbuf[mpar, b, 0:32], 64, 1) for b in (r, r + 4)]
            rows = jnp.concatenate([prods[0], prods[0], prods[1], prods[1]], axis=0)
            dots.append(jnp.sum(rows.T[0:64], axis=0, keepdims=True))
        gg = -(cross - 2.0 * jnp.concatenate(dots, axis=0) * veff * other) / (g * g)
        hh = swap(sq) / g
        left_lanes = lax.rem(wide, 64) < 32
        total = lambda p: jnp.sum(jnp.sum(p, axis=1, keepdims=True), axis=0, keepdims=True)
        mq = total(jnp.where(left_lanes, hh, 0.0)) / RANK
        mr = total(jnp.where(left_lanes, 0.0, hh)) / RANK
        mg = total(jnp.where(left_lanes, gg, 0.0)) / RANK
        k3_s[...] = g * jnp.exp(-STEP * (gg - mg))
        spread_all(fb_s, other * (2.0 * STEP * LOG2E) / g)
        spread_all(sb_s, (hh - jnp.where(left_lanes, mq, mr)) * (-STEP * LOG2E))
        spread_all(vb_s, veff)
        for b in range(NZ):
            m = mbuf[mpar, b, 0:32]
            turned = pltpu.roll(m, 64, 1)
            for side, first in ((0, turned), (1, m)):
                doubled_m = jnp.where(lane < 64, first, pltpu.roll(first, 64, 1))
                high, low = split(doubled_m * fb_s[b, 32 * side:32 * side + 32])
                w4_s[side, 32 * b:32 * b + 32, 0:128] = high
                w4_s[side, 32 * b:32 * b + 32, 128:256] = low
        for side in range(2):
            for t in range(tiles // 2):
                cols = slice(t * 256, (t + 1) * 256)
                f = jnp.dot(w4_s[side], x4_s[side, :, cols], preferred_element_type=jnp.float32)
                ua = jnp.concatenate(
                    [jnp.broadcast_to(u_s[side * tiles + 2 * t + i:side * tiles + 2 * t + i + 1, :], (32, 128)) for i in range(2)], axis=1
                )
                for b in range(NZ):
                    rows = slice(32 * side, 32 * side + 32)
                    s = sb_s[b, rows]
                    q = vb_s[b, rows]
                    e = jnp.exp2(f[32 * b:32 * b + 32] + jnp.concatenate([s, s], axis=1))
                    k_s[b, rows, cols] = k_s[b, rows, cols] * ua * jnp.concatenate([q, q], axis=1) * e

        v_s[...] = jnp.ones((4, 128), jnp.float32)
        vb_s[...] = jnp.ones((NZ, 64, 128), jnp.float32)
        base = outer * INNER

        def body(t, inner):
            plain_step(base + t)
            return inner

        lax.fori_loop(0, INNER - 1, body, 0)
        step = base + (INNER - 1)
        par = lax.rem(step, 2)
        u_of_rows()

        @pl.when(outer < MIRROR - 1)
        def _():
            start_moments()

        start_columns(par)

        @pl.when(outer < MIRROR - 1)
        def _():
            middle_moments()

        c, g, v = end_columns(par)
        g_s[...] = g
        veff_s[...] = v * sc_s[...]
        qs_s[...] = c * v
        npar = lax.rem(outer + 1, 2)

        @pl.when(outer < MIRROR - 1)
        def _():
            end_moments(npar, ())
            wait(mbuf.at[npar, 0:NZ - 1], msend.at[npar], mrecv.at[npar])

        return carry

    lax.fori_loop(0, MIRROR, mirror, 0)
    spread_all(vb_s, veff_s[...] * RANK)
    qv = vb_s[z]
    for t in range(tiles):
        lo_ref[:, tile(t)] = k_s[z, 0:half, tile(t)] * qv[0:half] * jnp.broadcast_to(u_s[t:t + 1, :], (half, 128))
        ro_ref[:, tile(t)] = k_s[z, half:2 * half, tile(t)] * qv[half:2 * half] * jnp.broadcast_to(
            u_s[tiles + t:tiles + t + 1, :], (half, 128))
    wo_ref[...] = g_s[...] * (RANK / total_count)


def shards(cloud_x, cloud_y, mass_x, mass_y, left_start, right_start, weight_start):
    ranks, points = left_start.shape
    total_count = float(points * lax.axis_size("dp"))
    tiles = points // 128
    f32 = jnp.float32
    bf16 = jnp.bfloat16
    dma = pltpu.SemaphoreType.DMA
    left, right, weights = pl.pallas_call(
        functools.partial(kernel, total_count),
        name="sinkhorn",
        out_shape=(
            jax.ShapeDtypeStruct((ranks, points), f32),
            jax.ShapeDtypeStruct((ranks, points), f32),
            jax.ShapeDtypeStruct((4, 128), f32),
        ),
        in_specs=[pl.BlockSpec(memory_space=pltpu.VMEM)] * 7,
        out_specs=[pl.BlockSpec(memory_space=pltpu.VMEM)] * 3,
        scratch_shapes=[
            pltpu.VMEM((NZ, 2 * ranks, points), f32),
            pltpu.VMEM((NZ, 2 * ranks, 128), f32),
            pltpu.VMEM((2 * ranks, points), f32),
            pltpu.VMEM((128, points), f32),
            pltpu.VMEM((2, 256, points), bf16),
            pltpu.VMEM((2, 256, 256), bf16),
            pltpu.VMEM((2 * tiles, 128), f32),
            pltpu.VMEM((2 * tiles, 128), f32),
            pltpu.VMEM((2 * tiles, 128), f32),
            pltpu.VMEM((NZ, 64, 128), f32),
            pltpu.VMEM((NZ, 64, 128), f32),
            pltpu.VMEM((NZ, 64, 128), f32),
            pltpu.VMEM((1, 128), f32),
            pltpu.VMEM((1, 128), f32),
            pltpu.VMEM((1, 128), f32),
            pltpu.VMEM((4, 128), f32),
            pltpu.VMEM((4, 128), f32),
            pltpu.VMEM((4, 128), f32),
            pltpu.VMEM((4, 128), f32),
            pltpu.VMEM((4, 128), f32),
            pltpu.VMEM((2, NZ, 2 * tiles, 128), f32),
            pltpu.VMEM((2, NDP, 1, 128), f32),
            pltpu.VMEM((2, NDP, 4, 128), f32),
            pltpu.VMEM((NX * NC, 40, 128), f32),
            pltpu.VMEM((NY, 40, 128), f32),
            pltpu.VMEM((2, NZ, 40, 128), f32),
            dma((2,)), dma((2,)), dma((2,)), dma((2,)), dma((2,)), dma((2,)),
            dma, dma, dma, dma, dma((2,)), dma((2,)),
            dma((NZ // 2, 2)), dma((NZ // 2, 2)),
        ],
        compiler_params=pltpu.CompilerParams(collective_id=0, has_side_effects=True),
    )(
        cloud_x, cloud_y, mass_x.reshape(tiles, 128), mass_y.reshape(tiles, 128),
        left_start, right_start, jnp.tile(weight_start, 4)[None],
    )
    z = lax.axis_index("rank")
    start = (lax.rem(z, 4) * 128 + lax.div(z, 4) * 64,)
    return left, right, lax.dynamic_slice(weights.reshape(512), start, (ranks,))


def solution(mesh):
    in_specs = (
        P(None, "dp"),
        P(None, "dp"),
        P("dp"),
        P("dp"),
        P("rank", "dp"),
        P("rank", "dp"),
        P("rank"),
    )
    out_specs = (P("rank", "dp"), P("rank", "dp"), P("rank"))
    return jax.shard_map(shards, mesh=mesh, in_specs=in_specs, out_specs=out_specs, check_vma=False)
```

```python
import functools

import jax
import jax.numpy as jnp
from jax import lax
from jax.experimental import pallas as pl
from jax.experimental.pallas import tpu as pltpu
from jax.sharding import PartitionSpec as P

RANK = 256
INNER = 4
MIRROR = 3
STEP = 2.0
MESH = pl.DeviceIdType.MESH
LOG2E = 1.4426950408889634

NX, NY, NC, NZ = 4, 8, 2, 8
NDP = NX * NY * NC


def far_first(n):
    return sorted(range(n), key=lambda d: -min(d, n - d))


DP_OFFSETS = sorted(
    [(dx, dy, dc) for dx in range(NX) for dy in range(NY) for dc in range(NC) if (dx, dy, dc) != (0, 0, 0)],
    key=lambda o: -(min(o[0], NX - o[0]) + min(o[1], NY - o[1])),
)
X_OFFSETS = [o for o in DP_OFFSETS if o[1] == 0 and o[2] == 0]
Y_OFFSETS = [o for o in DP_OFFSETS if o[0] == 0 and o[2] == 0]
Z_OFFSETS = [d for d in far_first(NZ) if d]


def cube_root(x):
    y = jnp.exp2(jnp.log2(x) * (1.0 / 3.0))
    y = y - (y - x / (y * y)) * (1.0 / 3.0)
    return jnp.where(x > 0.0, y, 0.0)


def split(x):
    high = x.astype(jnp.bfloat16)
    return high, (x - high.astype(jnp.float32)).astype(jnp.bfloat16)


def kernel(
    total_count,
    x_ref, y_ref, mx_ref, my_ref, left_ref, right_ref, w_ref,
    lo_ref, ro_ref, wo_ref,
    f_s, cl_s, m_s, k_s, cm_s, x4_s, w4_s, a_s, a1_s, n2_s, u_s, u1_s, uk_s, c_s, vb1_s, vb_s, fb_s, sb_s, o_s,
    v1_s, k1_s, sc_s, v_s, k3_s, g_s, veff_s, qs_s,
    zbuf, cbuf, dbuf, xbuf, ybuf, mbuf,
    zsend, zrecv, csend, crecv, dsend, drecv, xsend, xrecv, ysend, yrecv, msend, mrecv, asend, arecv, psend, precv,
):
    dp = lax.axis_index("dp")
    z = lax.axis_index("rank")
    core = lax.rem(dp, NC)
    twin = 1 - core
    yy = lax.rem(lax.div(dp, NC), NY)
    xx = lax.div(dp, NC * NY)
    chip = lax.div(dp, NC)
    tiles = left_ref.shape[1] // 128
    f32 = jnp.float32

    def dp_target(o):
        tx = lax.rem(xx + o[0], NX)
        ty = lax.rem(yy + o[1], NY)
        tc = lax.rem(core + o[2], NC)
        return ((tx * NY + ty) * NC + tc, z)

    def z_target(d):
        return (dp, lax.rem(z + d, NZ))

    def zc_target(d):
        return (chip * NC + twin, lax.rem(z + d, NZ))

    partner = (chip * NC + twin, z)
    z_targets = [z_target(d) for d in Z_OFFSETS]
    zc_targets = [t(d) for d in Z_OFFSETS for t in (zc_target, z_target)] + [partner]

    barrier = pltpu.get_barrier_semaphore()
    for d in Z_OFFSETS:
        pl.semaphore_signal(barrier, inc=1, device_id=z_target(d), device_id_type=MESH)
        pl.semaphore_signal(barrier, inc=1, device_id=zc_target(d), device_id_type=MESH)
    for o in DP_OFFSETS:
        pl.semaphore_signal(barrier, inc=1, device_id=dp_target(o), device_id_type=MESH)

    def send(slot, targets, ssem, rsem):
        for t in targets:
            pltpu.make_async_remote_copy(
                src_ref=slot, dst_ref=slot, send_sem=ssem, recv_sem=rsem, device_id=t, device_id_type=MESH
            ).start()

    def wait(some, ssem, rsem):
        pltpu.make_async_copy(some, some, rsem).wait()
        pltpu.make_async_copy(some, some, ssem).wait()

    def pair(i):
        src, dst = (
            (f_s.at[twin], k_s.at[z, core]),
            (m_s.at[twin], a_s.at[core]),
            (cl_s.at[twin], cm_s.at[core]),
            (u1_s.at[twin], u_s.at[core]),
            (o_s.at[0], o_s.at[1]),
        )[i]
        return pltpu.make_async_remote_copy(
            src_ref=src, dst_ref=dst, send_sem=psend.at[i], recv_sem=precv.at[i], device_id=partner, device_id_type=MESH
        )

    def end_pair(i):
        pair(i).wait_recv()
        pair(i).wait_send()

    def tile(t):
        return slice(t * 128, (t + 1) * 128)

    f_s[0] = left_ref[...]
    f_s[1] = right_ref[...]
    cl_s[0] = x_ref[...]
    cl_s[1] = y_ref[...]
    m_s[0] = mx_ref[...]
    m_s[1] = my_ref[...]
    a1_s[0:tiles, :] = mx_ref[...]
    a1_s[tiles:2 * tiles, :] = my_ref[...]
    lane = lax.broadcasted_iota(jnp.int32, (1, 128), 1)
    pl.semaphore_wait(barrier, 2 * len(Z_OFFSETS) + len(DP_OFFSETS))
    for i in range(3):
        pair(i).start()
    k_s[z, core] = f_s[core]
    a_s[core] = m_s[core]
    cm_s[core] = cl_s[core]

    def spread(vec):
        return jnp.broadcast_to(vec, (128, 128)).T

    def spread_all(dst, vec):
        for h in range(2):
            dst[h] = spread(vec[h:h + 1]).reshape(NZ, 16, 128)

    def gather_rows(rows):
        return jnp.sum(rows.T, axis=0, keepdims=True)

    def swap(p):
        return jnp.where(lax.rem(lane, 64) < 32, pltpu.roll(p, 96, 1), pltpu.roll(p, 32, 1))

    def doubled(c):
        return jnp.where(lane < 64, c, pltpu.roll(c, 64, 1))

    def ring_copies(i):
        hop, late = divmod(i, 2)
        copies = []
        for way, sign in ((0, 1), (1, -1)):
            part = k_s.at[lax.rem(z - sign * hop + NZ, NZ), (way + late) % 2]
            copies.append(pltpu.make_async_remote_copy(
                src_ref=part, dst_ref=part, send_sem=asend.at[i, way], recv_sem=arecv.at[i, way],
                device_id=(dp, lax.rem(z + sign + NZ, NZ)), device_id_type=MESH,
            ))
        return copies

    def ring_end(i):
        for copy in ring_copies(i):
            copy.wait_recv()
            copy.wait_send()

    def ring(i):
        if i >= 2:
            ring_end(i - 2)
        for copy in ring_copies(i):
            copy.start()

    def at(step, when, action):
        @pl.when(step == when)
        def _():
            action()

    def row_sums(step):
        par = lax.rem(step, 2)
        for t in range(tiles):
            for side in range(2):
                i = side * tiles + t
                b = f_s[side, :, tile(t)] * vb1_s[32 * side:32 * side + 32]
                zbuf[par, z, i:i + 1, :] = jnp.sum(b, axis=0, keepdims=True)
        send(zbuf.at[par, z], z_targets, zsend.at[par], zrecv.at[par])

        def first():
            end_pair(0)
            ring(0)
            end_pair(1)
            end_pair(2)
            prepare()

        at(step, 0, first)
        at(step, 2, lambda: ring(3))
        at(step, 3, lambda: ring(5))
        wait(zbuf.at[par, 0:NZ - 1], zsend.at[par], zrecv.at[par])
        total = zbuf[par, 0]
        for i in range(1, NZ):
            total = total + zbuf[par, i]
        u = a1_s[...] / total
        u1_s[0] = u[0:tiles]
        u1_s[1] = u[tiles:2 * tiles]

    def prepare():
        for s in range(2):
            for t in range(tiles):
                b = cm_s[s, :, tile(t)]
                n2_s[s, t:t + 1, :] = jnp.sum(b * b, axis=0, keepdims=True)
                high, low = split(b)
                both = jnp.concatenate([high, low], axis=0)
                x4_s[s, 0:128, tile(t)] = both
                x4_s[s, 128:256, tile(t)] = both

    def own_columns():
        accs = []
        for side in range(2):
            acc = jnp.zeros((32, 128), f32)
            for t in range(tiles):
                acc = acc + f_s[side, :, tile(t)] * jnp.broadcast_to(u1_s[side, t:t + 1, :], (32, 128))
            accs.append(acc)
        return accs

    def summed(buf, par, first, count):
        parts = [buf[par, first + i] for i in range(4)]
        for i in range(4, count):
            parts[i % 4] = parts[i % 4] + buf[par, first + i]
        return (parts[0] + parts[1]) + (parts[2] + parts[3])

    def exchange_first(par, low, high):
        cbuf[par, dp] = gather_rows(jnp.concatenate(low + high, axis=0))
        send(cbuf.at[par, dp], [dp_target(o) for o in DP_OFFSETS], csend.at[par], crecv.at[par])

    def rescale_first(c):
        v = v1_s[...]
        p = v * c
        g = cube_root(k1_s[...] * (p * swap(p)))
        v = g / c
        v1_s[...] = v
        return g, v

    def first_step(step, carry):
        par = lax.rem(step, 2)
        row_sums(step)
        ax = jnp.sum(a1_s[0:tiles, :], axis=0, keepdims=True)
        ay = jnp.sum(a1_s[tiles:2 * tiles, :], axis=0, keepdims=True)
        exchange_first(par, own_columns(), [jnp.broadcast_to(ax, (32, 128)), jnp.broadcast_to(ay, (32, 128))])
        at(step, 0, lambda: ring(1))
        at(step, 1, lambda: ring(2))
        at(step, 2, lambda: ring(4))
        wait(cbuf.at[par, 0:NDP - 1], csend.at[par], crecv.at[par])
        c = summed(cbuf, par, 0, NDP)
        scale = total_count / jnp.where(lane >= 64, c, pltpu.roll(c, 64, 1))
        sc_s[...] = scale
        g, v = rescale_first(doubled(c) * scale)
        vb1_s[...] = spread(v)[0:64]
        return carry

    def placed(row, offset):
        moved = pltpu.roll(jnp.broadcast_to(row, (8, 128)), lax.rem(z * 16 - offset + 256, 128), 1)[0:1]
        return jnp.where((lane >= z * 16) & (lane < z * 16 + 16), moved, 0.0)

    def start_moments():
        acc = jnp.zeros((32, 128), f32)
        both = jnp.zeros((32, 128), f32)
        for s in range(2):
            for t in range(tiles):
                b = k_s[z, s, :, tile(t)] * jnp.broadcast_to(u_s[s, t:t + 1, :], (32, 128))
                acc = acc + b * jnp.broadcast_to(n2_s[s, t:t + 1, :], (32, 128))
                high, low = split(b)
                uk_s[0:32, tile(t)] = high
                uk_s[32:64, tile(t)] = low
            d = lax.dot_general(
                uk_s[...], x4_s[s, 0:128, :], (((1,), (1,)), ((), ())), preferred_element_type=f32
            )
            both = both + d[0:32] + d[32:64]
        both = both + pltpu.roll(both, 64, 1)
        xbuf[xx, 0:16] = jnp.where(lane < 64, both[0:16], both[16:32])
        sums = gather_rows(jnp.concatenate([acc] * 4, axis=0))
        xbuf[xx, 16:17] = placed(sums, 0)
        xbuf[xx, 17:18] = placed(sums, 16)
        xbuf[xx, 18:24] = jnp.zeros((6, 128), f32)
        send(xbuf.at[xx], [dp_target(o) for o in X_OFFSETS], xsend, xrecv)

    def middle_moments():
        wait(xbuf.at[0:NX - 1], xsend, xrecv)
        m = xbuf[0]
        for i in range(1, NX):
            m = m + xbuf[i]
        ybuf[yy] = m
        send(ybuf.at[yy], [dp_target(o) for o in Y_OFFSETS], ysend, yrecv)

    def end_moments(par, rows):
        wait(ybuf.at[0:NY - 1], ysend, yrecv)
        m = ybuf[0]
        for i in range(1, NY):
            m = m + ybuf[i]
        slot = mbuf.at[par, core * NZ + z]
        slot[...] = m
        for i, row in enumerate(rows):
            slot[18 + i:19 + i] = row
        send(slot, zc_targets, msend.at[par], mrecv.at[par])

    v1_s[...] = jnp.ones((1, 128), f32)
    k1_s[...] = w_ref[...]
    vb1_s[...] = jnp.ones((64, 128), f32)
    lax.fori_loop(0, INNER - 1, first_step, 0)
    par = (INNER - 1) % 2
    row_sums(jnp.int32(INNER - 1))
    pair(3).start()
    u_s[core] = u1_s[core]
    accs = own_columns()
    exchange_first(par, accs, accs)
    end_pair(3)
    start_moments()
    ring(6)
    middle_moments()
    wait(cbuf.at[par, 0:NDP - 1], csend.at[par], crecv.at[par])
    c1 = summed(cbuf, par, 0, NDP) * sc_s[...]
    g1, v1 = rescale_first(c1)
    mine = core * 32
    e1 = v1 * sc_s[...]
    q1 = c1 * v1
    end_moments(0, [placed(p, mine + 16 * h) for p in (g1, e1, q1) for h in range(2)])
    ring_end(5)
    ring_end(6)
    wait(mbuf.at[0, 0:2 * NZ - 1], msend.at[0], mrecv.at[0])

    def over_blocks(par, cloud, first):
        rows = mbuf[par, cloud * NZ, first:first + 2]
        for b in range(1, NZ):
            rows = rows + mbuf[par, cloud * NZ + b, first:first + 2]
        return rows

    g_s[...] = over_blocks(0, core, 18)
    for i, cloud in enumerate((core, twin)):
        veff_s[i] = over_blocks(0, cloud, 20)
        qs_s[i] = over_blocks(0, cloud, 22)
    scales = [jnp.where(core == c, sc_s[...], pltpu.roll(sc_s[...], 32, 1)) for c in (0, 1)]
    for i in range(2):
        first = jnp.sum(jnp.where(lane == 0, scales[i], 0.0), axis=1, keepdims=True)
        a1_s[i:i + 1, :] = jnp.broadcast_to(first, (1, 128))

    def u_of_rows():
        for s in range(2):
            def body(b, accs):
                accs = list(accs)
                for j in range(4):
                    v = vb_s[j // 2, b, 8 * (j % 2):8 * (j % 2) + 8]
                    for t in range(tiles):
                        accs[t] = accs[t] + k_s[b, s, 8 * j:8 * j + 8, tile(t)] * v
                return tuple(accs)

            accs = lax.fori_loop(0, NZ, body, tuple(jnp.zeros((8, 128), f32) for _ in range(tiles)))
            for t in range(tiles):
                u_s[s, t:t + 1, :] = a_s[s, t:t + 1, :] / jnp.sum(accs[t], axis=0, keepdims=True)

    def start_columns(par):
        us = [[jnp.broadcast_to(u_s[s, t:t + 1, :], (8, 128)) for t in range(tiles)] for s in range(2)]

        def body(b, carry):
            for j in range(4):
                acc = [k_s[b, s, 8 * j:8 * j + 8, tile(t)] * us[s][t] for s in range(2) for t in range(tiles)]
                while len(acc) > 1:
                    acc = [p + q for p, q in zip(acc[::2], acc[1::2])]
                c_s[j // 2, b, 8 * (j % 2):8 * (j % 2) + 8] = acc[0]
            return carry

        lax.fori_loop(0, NZ, body, 0)
        slot = dbuf.at[par, core * (NDP // 2) + chip]
        slot[...] = jnp.concatenate([gather_rows(c_s[h].reshape(128, 128)) for h in range(2)], axis=0)
        send(slot, [dp_target(o) for o in DP_OFFSETS], dsend.at[par], drecv.at[par])

    def end_columns(par):
        wait(dbuf.at[par, 0:NDP - 1], dsend.at[par], drecv.at[par])
        c = [summed(dbuf, par, cloud * (NDP // 2), NDP // 2) * a1_s[i:i + 1] for i, cloud in enumerate((core, twin))]
        g = cube_root(k3_s[...] * ((v_s[0] * c[0]) * (v_s[1] * c[1])))
        for i in range(2):
            v_s[i] = g / c[i]
        return c, g

    def plain_step(step):
        par = lax.rem(step, 2)
        u_of_rows()
        start_columns(par)
        end_columns(par)
        spread_all(vb_s, v_s[0])

    def mirror(outer, carry):
        mpar = lax.rem(outer, 2)
        g = g_s[...]
        sq = [over_blocks(mpar, cloud, 16) * veff_s[i] for i, cloud in enumerate((core, twin))]
        cross = sq[0] * qs_s[1] + sq[1] * qs_s[0]
        prod = jnp.concatenate([mbuf[mpar, b, 0:16] * mbuf[mpar, NZ + b, 0:16] for b in range(NZ)], axis=0).T
        dots = jnp.concatenate([jnp.sum(prod[64 * h:64 * h + 64], axis=0, keepdims=True) for h in range(2)], axis=0)
        gg = -(cross - 2.0 * dots * (veff_s[0] * veff_s[1])) / (g * g)
        hh = sq[1] / g

        def mean(p):
            return jnp.sum(jnp.sum(p, axis=1, keepdims=True), axis=0, keepdims=True) / RANK

        k3_s[...] = g * jnp.exp(-STEP * (gg - mean(gg)))
        spread_all(fb_s, veff_s[1] * (2.0 * STEP * LOG2E) / g)
        spread_all(sb_s, (hh - mean(hh)) * (-STEP * LOG2E))
        spread_all(vb_s, veff_s[0])
        for b in range(NZ):
            m = mbuf[mpar, twin * NZ + b, 0:16]
            turned = pltpu.roll(m, 64, 1)
            for h, pair_of in ((0, jnp.where(lane < 64, m, turned)), (1, jnp.where(lane < 64, turned, m))):
                high, low = split(pair_of * fb_s[h, b])
                w4_s[32 * b + 16 * h:32 * b + 16 * h + 16, 0:128] = high
                w4_s[32 * b + 16 * h:32 * b + 16 * h + 16, 128:256] = low
        for s in range(2):
            for t in range(tiles // 2):
                cols = slice(t * 256, (t + 1) * 256)
                f = jnp.dot(w4_s[...], x4_s[s, :, cols], preferred_element_type=f32)
                ua = jnp.concatenate(
                    [jnp.broadcast_to(u_s[s, 2 * t + i:2 * t + i + 1, :], (16, 128)) for i in range(2)], axis=1
                )
                for b in range(NZ):
                    for h in range(2):
                        rows = slice(16 * h, 16 * h + 16)
                        sh = sb_s[h, b]
                        q = vb_s[h, b]
                        e = jnp.exp2(f[32 * b + 16 * h:32 * b + 16 * h + 16] + jnp.concatenate([sh, sh], axis=1))
                        k_s[b, s, rows, cols] = k_s[b, s, rows, cols] * ua * jnp.concatenate([q, q], axis=1) * e

        v_s[...] = jnp.ones((2, 2, 128), f32)
        vb_s[...] = jnp.ones((2, NZ, 16, 128), f32)
        base = outer * INNER

        def body(t, inner):
            plain_step(base + t)
            return inner

        lax.fori_loop(0, INNER - 1, body, 0)
        par = lax.rem(base + (INNER - 1), 2)
        npar = lax.rem(outer + 1, 2)
        u_of_rows()

        @pl.when(outer < MIRROR - 1)
        def _():
            start_moments()

        start_columns(par)

        @pl.when(outer < MIRROR - 1)
        def _():
            middle_moments()

        c, g = end_columns(par)
        g_s[...] = g
        for i in range(2):
            veff_s[i] = v_s[i] * a1_s[i:i + 1]
            qs_s[i] = c[i] * v_s[i]

        @pl.when(outer < MIRROR - 1)
        def _():
            end_moments(npar, ())
            wait(mbuf.at[npar, 0:2 * NZ - 1], msend.at[npar], mrecv.at[npar])

        return carry

    lax.fori_loop(0, MIRROR, mirror, 0)
    spread_all(vb_s, veff_s[0] * RANK)

    def result(s, t):
        q = jnp.concatenate([vb_s[0, z], vb_s[1, z]], axis=0)
        return k_s[z, s, :, tile(t)] * q * jnp.broadcast_to(u_s[s, t:t + 1, :], (32, 128))

    for t in range(tiles):
        o_s[0, :, tile(t)] = result(twin, t)
    pair(4).start()
    wo_ref[...] = g_s[...] * (RANK / total_count)
    for side, first, second in ((0, lo_ref, ro_ref), (1, ro_ref, lo_ref)):
        @pl.when(core == side)
        def _():
            for t in range(tiles):
                first[:, tile(t)] = result(core, t)
            end_pair(4)
            second[...] = o_s[1]


def shards(cloud_x, cloud_y, mass_x, mass_y, left_start, right_start, weight_start):
    ranks, points = left_start.shape
    total_count = float(points * lax.axis_size("dp"))
    tiles = points // 128
    f32 = jnp.float32
    bf16 = jnp.bfloat16
    dma = pltpu.SemaphoreType.DMA
    left, right, weights = pl.pallas_call(
        functools.partial(kernel, total_count),
        name="sinkhorn",
        out_shape=(
            jax.ShapeDtypeStruct((ranks, points), f32),
            jax.ShapeDtypeStruct((ranks, points), f32),
            jax.ShapeDtypeStruct((2, 128), f32),
        ),
        in_specs=[pl.BlockSpec(memory_space=pltpu.VMEM)] * 7,
        out_specs=[pl.BlockSpec(memory_space=pltpu.VMEM)] * 3,
        scratch_shapes=[
            pltpu.VMEM((2, ranks, points), f32),
            pltpu.VMEM((2, 64, points), f32),
            pltpu.VMEM((2, tiles, 128), f32),
            pltpu.VMEM((NZ, 2, ranks, points), f32),
            pltpu.VMEM((2, 64, points), f32),
            pltpu.VMEM((2, 256, points), bf16),
            pltpu.VMEM((256, 256), bf16),
            pltpu.VMEM((2, tiles, 128), f32),
            pltpu.VMEM((2 * tiles, 128), f32),
            pltpu.VMEM((2, tiles, 128), f32),
            pltpu.VMEM((2, tiles, 128), f32),
            pltpu.VMEM((2, tiles, 128), f32),
            pltpu.VMEM((64, points), bf16),
            pltpu.VMEM((2, NZ, 16, 128), f32),
            pltpu.VMEM((64, 128), f32),
            pltpu.VMEM((2, NZ, 16, 128), f32),
            pltpu.VMEM((2, NZ, 16, 128), f32),
            pltpu.VMEM((2, NZ, 16, 128), f32),
            pltpu.VMEM((2, ranks, points), f32),
            pltpu.VMEM((1, 128), f32),
            pltpu.VMEM((1, 128), f32),
            pltpu.VMEM((1, 128), f32),
            pltpu.VMEM((2, 2, 128), f32),
            pltpu.VMEM((2, 128), f32),
            pltpu.VMEM((2, 128), f32),
            pltpu.VMEM((2, 2, 128), f32),
            pltpu.VMEM((2, 2, 128), f32),
            pltpu.VMEM((2, NZ, 2 * tiles, 128), f32),
            pltpu.VMEM((2, NDP, 1, 128), f32),
            pltpu.VMEM((2, NDP, 2, 128), f32),
            pltpu.VMEM((NX, 24, 128), f32),
            pltpu.VMEM((NY, 24, 128), f32),
            pltpu.VMEM((2, 2 * NZ, 24, 128), f32),
            dma((2,)), dma((2,)), dma((2,)), dma((2,)), dma((2,)), dma((2,)),
            dma, dma, dma, dma, dma((2,)), dma((2,)),
            dma((NZ - 1, 2)), dma((NZ - 1, 2)), dma((5,)), dma((5,)),
        ],
        compiler_params=pltpu.CompilerParams(collective_id=0, has_side_effects=True),
    )(
        cloud_x, cloud_y, mass_x.reshape(tiles, 128), mass_y.reshape(tiles, 128),
        left_start, right_start, jnp.tile(weight_start, 4)[None],
    )
    z = lax.axis_index("rank")
    own = lax.dynamic_slice(weights.reshape(2, NZ, 16), (0, z, 0), (2, 1, 16))
    return left, right, own.reshape(ranks)


def solution(mesh):
    in_specs = (
        P(None, "dp"),
        P(None, "dp"),
        P("dp"),
        P("dp"),
        P("rank", "dp"),
        P("rank", "dp"),
        P("rank"),
    )
    out_specs = (P("rank", "dp"), P("rank", "dp"), P("rank"))
    return jax.shard_map(shards, mesh=mesh, in_specs=in_specs, out_specs=out_specs, check_vma=False)
```

```python
import functools

import jax
import jax.numpy as jnp
from jax import lax
from jax.experimental import pallas as pl
from jax.experimental.pallas import tpu as pltpu
from jax.sharding import PartitionSpec as P

RANK = 256
INNER = 4
MIRROR = 3
STEP = 2.0
MESH = pl.DeviceIdType.MESH
LOG2E = 1.4426950408889634

NX, NY, NC, NZ = 4, 8, 2, 8
NDP = NX * NY * NC


def far_first(n):
    return sorted(range(n), key=lambda d: -min(d, n - d))


DP_OFFSETS = sorted(
    [(dx, dy, dc) for dx in range(NX) for dy in range(NY) for dc in range(NC) if (dx, dy, dc) != (0, 0, 0)],
    key=lambda o: -(min(o[0], NX - o[0]) + min(o[1], NY - o[1])),
)
X_OFFSETS = [o for o in DP_OFFSETS if o[1] == 0 and o[2] == 0]
Y_OFFSETS = [o for o in DP_OFFSETS if o[0] == 0 and o[2] == 0]
Z_OFFSETS = [d for d in far_first(NZ) if d]


def cube_root(x):
    y = jnp.exp2(jnp.log2(x) * (1.0 / 3.0))
    y = y - (y - x / (y * y)) * (1.0 / 3.0)
    return jnp.where(x > 0.0, y, 0.0)


def split(x):
    high = x.astype(jnp.bfloat16)
    return high, (x - high.astype(jnp.float32)).astype(jnp.bfloat16)


def kernel(
    total_count,
    x_ref, y_ref, mx_ref, my_ref, left_ref, right_ref, w_ref,
    ku_ref, vo_ref, wo_ref,
    w_s, f_s, cl_s, m_s, k_s, cm_s, x4_s, w4_s, a_s, a1_s, n2_s, u_s, u1_s, uk_s, c_s, vb1_s, vb_s, fb_s, sb_s, o_s, ou_s, ku_s,
    v1_s, k1_s, sc_s, v_s, k3_s, g_s, veff_s, qs_s,
    zbuf, cbuf, dbuf, xbuf, ybuf, mbuf,
    zsend, zrecv, csend, crecv, dsend, drecv, xsend, xrecv, ysend, yrecv, msend, mrecv, asend, arecv, psend, precv, isem,
):
    dp = lax.axis_index("dp")
    z = lax.axis_index("rank")
    core = lax.rem(dp, NC)
    twin = 1 - core
    yy = lax.rem(lax.div(dp, NC), NY)
    xx = lax.div(dp, NC * NY)
    chip = lax.div(dp, NC)
    tiles = mx_ref.shape[0]
    f32 = jnp.float32

    def dp_target(o):
        tx = lax.rem(xx + o[0], NX)
        ty = lax.rem(yy + o[1], NY)
        tc = lax.rem(core + o[2], NC)
        return ((tx * NY + ty) * NC + tc, z)

    def z_target(d):
        return (dp, lax.rem(z + d, NZ))

    def zc_target(d):
        return (chip * NC + twin, lax.rem(z + d, NZ))

    partner = (chip * NC + twin, z)
    z_targets = [z_target(d) for d in Z_OFFSETS]
    zc_targets = [t(d) for d in Z_OFFSETS for t in (zc_target, z_target)] + [partner]

    barrier = pltpu.get_barrier_semaphore()
    for d in Z_OFFSETS:
        pl.semaphore_signal(barrier, inc=1, device_id=z_target(d), device_id_type=MESH)
        pl.semaphore_signal(barrier, inc=1, device_id=zc_target(d), device_id_type=MESH)
    for o in DP_OFFSETS:
        pl.semaphore_signal(barrier, inc=1, device_id=dp_target(o), device_id_type=MESH)

    def send(slot, targets, ssem, rsem):
        for t in targets:
            pltpu.make_async_remote_copy(
                src_ref=slot, dst_ref=slot, send_sem=ssem, recv_sem=rsem, device_id=t, device_id_type=MESH
            ).start()

    def wait(some, ssem, rsem):
        pltpu.make_async_copy(some, some, rsem).wait()
        pltpu.make_async_copy(some, some, ssem).wait()

    def pair(i):
        src, dst = (
            (f_s.at[twin], k_s.at[z, core]),
            (m_s.at[twin], a_s.at[core]),
            (cl_s.at[twin], cm_s.at[core]),
            (u1_s.at[twin], u_s.at[core]),
            (k_s.at[z, twin], o_s),
            (u_s.at[twin], ou_s),
        )[i]
        return pltpu.make_async_remote_copy(
            src_ref=src, dst_ref=dst, send_sem=psend.at[i], recv_sem=precv.at[i], device_id=partner, device_id_type=MESH
        )

    def scaled():
        return pltpu.make_async_copy(ku_s, ku_ref, isem.at[7])

    def end_pair(i):
        pair(i).wait_recv()
        pair(i).wait_send()

    def tile(t):
        return slice(t * 128, (t + 1) * 128)

    inputs = [
        pltpu.make_async_copy(src, dst, isem.at[i])
        for i, (src, dst) in enumerate((
            (left_ref, f_s.at[0]), (right_ref, f_s.at[1]), (mx_ref, m_s.at[0]), (my_ref, m_s.at[1]),
            (x_ref, cl_s.at[0]), (y_ref, cl_s.at[1]), (w_ref, w_s),
        ))
    ]
    for copy in inputs:
        copy.start()
    lane = lax.broadcasted_iota(jnp.int32, (1, 128), 1)
    for copy in inputs:
        copy.wait()
    a1_s[0:tiles, :] = m_s[0]
    a1_s[tiles:2 * tiles, :] = m_s[1]
    k_s[z, core] = f_s[core]
    a_s[core] = m_s[core]
    cm_s[core] = cl_s[core]
    k1_s[0:1, 0:w_s.shape[1]] = w_s[...]
    start = jnp.where(lane < 32, k1_s[...], 0.0)
    start = start + pltpu.roll(start, 32, 1)
    k1_s[...] = start + pltpu.roll(start, 64, 1)
    pl.semaphore_wait(barrier, 2 * len(Z_OFFSETS) + len(DP_OFFSETS))
    for i in range(3):
        pair(i).start()

    def spread(vec):
        return jnp.broadcast_to(vec, (128, 128)).T

    def spread_all(dst, vec):
        for h in range(2):
            dst[h] = spread(vec[h:h + 1]).reshape(NZ, 16, 128)

    def gather_rows(rows):
        return jnp.sum(rows.T, axis=0, keepdims=True)

    def swap(p):
        return jnp.where(lax.rem(lane, 64) < 32, pltpu.roll(p, 96, 1), pltpu.roll(p, 32, 1))

    def doubled(c):
        return jnp.where(lane < 64, c, pltpu.roll(c, 64, 1))

    def ring_copies(i):
        hop, late = divmod(i, 2)
        copies = []
        for way, sign in ((0, 1), (1, -1)):
            part = k_s.at[lax.rem(z - sign * hop + NZ, NZ), (way + late) % 2]
            copies.append(pltpu.make_async_remote_copy(
                src_ref=part, dst_ref=part, send_sem=asend.at[i, way], recv_sem=arecv.at[i, way],
                device_id=(dp, lax.rem(z + sign + NZ, NZ)), device_id_type=MESH,
            ))
        return copies

    def ring_end(i):
        for copy in ring_copies(i):
            copy.wait_recv()
            copy.wait_send()

    def ring(i):
        if i >= 2:
            ring_end(i - 2)
        for copy in ring_copies(i):
            copy.start()

    def at(step, when, action):
        @pl.when(step == when)
        def _():
            action()

    def row_sums(step):
        par = lax.rem(step, 2)
        for t in range(tiles):
            for side in range(2):
                i = side * tiles + t
                b = f_s[side, :, tile(t)] * vb1_s[32 * side:32 * side + 32]
                zbuf[par, z, i:i + 1, :] = jnp.sum(b, axis=0, keepdims=True)
        send(zbuf.at[par, z], z_targets, zsend.at[par], zrecv.at[par])

        def first():
            end_pair(0)
            ring(0)
            end_pair(1)
            end_pair(2)
            prepare()

        at(step, 0, first)
        at(step, 2, lambda: ring(3))
        at(step, 3, lambda: ring(5))
        wait(zbuf.at[par, 0:NZ - 1], zsend.at[par], zrecv.at[par])
        total = zbuf[par, 0]
        for i in range(1, NZ):
            total = total + zbuf[par, i]
        u = a1_s[...] / total
        u1_s[0] = u[0:tiles]
        u1_s[1] = u[tiles:2 * tiles]

    def prepare():
        for s in range(2):
            for t in range(tiles):
                b = cm_s[s, :, tile(t)]
                n2_s[s, t:t + 1, :] = jnp.sum(b * b, axis=0, keepdims=True)
                high, low = split(b)
                both = jnp.concatenate([high, low], axis=0)
                x4_s[s, 0:128, tile(t)] = both
                x4_s[s, 128:256, tile(t)] = both

    def own_columns():
        accs = []
        for side in range(2):
            acc = jnp.zeros((32, 128), f32)
            for t in range(tiles):
                acc = acc + f_s[side, :, tile(t)] * jnp.broadcast_to(u1_s[side, t:t + 1, :], (32, 128))
            accs.append(acc)
        return accs

    def summed(buf, par, first, count):
        parts = [buf[par, first + i] for i in range(4)]
        for i in range(4, count):
            parts[i % 4] = parts[i % 4] + buf[par, first + i]
        return (parts[0] + parts[1]) + (parts[2] + parts[3])

    def exchange_first(par, low, high):
        cbuf[par, dp] = gather_rows(jnp.concatenate(low + high, axis=0))
        send(cbuf.at[par, dp], [dp_target(o) for o in DP_OFFSETS], csend.at[par], crecv.at[par])

    def rescale_first(c):
        v = v1_s[...]
        p = v * c
        g = cube_root(k1_s[...] * (p * swap(p)))
        v = g / c
        v1_s[...] = v
        return g, v

    def first_step(step, carry):
        par = lax.rem(step, 2)
        row_sums(step)
        ax = jnp.sum(a1_s[0:tiles, :], axis=0, keepdims=True)
        ay = jnp.sum(a1_s[tiles:2 * tiles, :], axis=0, keepdims=True)
        exchange_first(par, own_columns(), [jnp.broadcast_to(ax, (32, 128)), jnp.broadcast_to(ay, (32, 128))])
        at(step, 0, lambda: ring(1))
        at(step, 1, lambda: ring(2))
        at(step, 2, lambda: ring(4))
        wait(cbuf.at[par, 0:NDP - 1], csend.at[par], crecv.at[par])
        c = summed(cbuf, par, 0, NDP)
        scale = total_count / jnp.where(lane >= 64, c, pltpu.roll(c, 64, 1))
        sc_s[...] = scale
        g, v = rescale_first(doubled(c) * scale)
        vb1_s[...] = spread(v)[0:64]
        return carry

    def placed(row, offset):
        moved = pltpu.roll(jnp.broadcast_to(row, (8, 128)), lax.rem(z * 16 - offset + 256, 128), 1)[0:1]
        return jnp.where((lane >= z * 16) & (lane < z * 16 + 16), moved, 0.0)

    def start_moments():
        acc = jnp.zeros((32, 128), f32)
        both = jnp.zeros((32, 128), f32)
        for s in range(2):
            for t in range(tiles):
                b = k_s[z, s, :, tile(t)] * jnp.broadcast_to(u_s[s, t:t + 1, :], (32, 128))
                acc = acc + b * jnp.broadcast_to(n2_s[s, t:t + 1, :], (32, 128))
                high, low = split(b)
                uk_s[0:32, tile(t)] = high
                uk_s[32:64, tile(t)] = low
            d = lax.dot_general(
                uk_s[...], x4_s[s, 0:128, :], (((1,), (1,)), ((), ())), preferred_element_type=f32
            )
            both = both + d[0:32] + d[32:64]
        both = both + pltpu.roll(both, 64, 1)
        xbuf[xx, 0:16] = jnp.where(lane < 64, both[0:16], both[16:32])
        sums = gather_rows(jnp.concatenate([acc] * 4, axis=0))
        xbuf[xx, 16:17] = placed(sums, 0)
        xbuf[xx, 17:18] = placed(sums, 16)
        xbuf[xx, 18:24] = jnp.zeros((6, 128), f32)
        send(xbuf.at[xx], [dp_target(o) for o in X_OFFSETS], xsend, xrecv)

    def middle_moments():
        wait(xbuf.at[0:NX - 1], xsend, xrecv)
        m = xbuf[0]
        for i in range(1, NX):
            m = m + xbuf[i]
        ybuf[yy] = m
        send(ybuf.at[yy], [dp_target(o) for o in Y_OFFSETS], ysend, yrecv)

    def end_moments(par, rows):
        wait(ybuf.at[0:NY - 1], ysend, yrecv)
        m = ybuf[0]
        for i in range(1, NY):
            m = m + ybuf[i]
        slot = mbuf.at[par, core * NZ + z]
        slot[...] = m
        for i, row in enumerate(rows):
            slot[18 + i:19 + i] = row
        send(slot, zc_targets, msend.at[par], mrecv.at[par])

    v1_s[...] = jnp.ones((1, 128), f32)
    vb1_s[...] = jnp.ones((64, 128), f32)
    lax.fori_loop(0, INNER - 1, first_step, 0)
    par = (INNER - 1) % 2
    row_sums(jnp.int32(INNER - 1))
    pair(3).start()
    u_s[core] = u1_s[core]
    accs = own_columns()
    exchange_first(par, accs, accs)
    end_pair(3)
    start_moments()
    ring(6)
    middle_moments()
    wait(cbuf.at[par, 0:NDP - 1], csend.at[par], crecv.at[par])
    c1 = summed(cbuf, par, 0, NDP) * sc_s[...]
    g1, v1 = rescale_first(c1)
    mine = core * 32
    e1 = v1 * sc_s[...]
    q1 = c1 * v1
    end_moments(0, [placed(p, mine + 16 * h) for p in (g1, e1, q1) for h in range(2)])
    ring_end(5)
    ring_end(6)
    wait(mbuf.at[0, 0:2 * NZ - 1], msend.at[0], mrecv.at[0])

    def over_blocks(par, cloud, first):
        rows = mbuf[par, cloud * NZ, first:first + 2]
        for b in range(1, NZ):
            rows = rows + mbuf[par, cloud * NZ + b, first:first + 2]
        return rows

    g_s[...] = over_blocks(0, core, 18)
    for i, cloud in enumerate((core, twin)):
        veff_s[i] = over_blocks(0, cloud, 20)
        qs_s[i] = over_blocks(0, cloud, 22)
    scales = [jnp.where(core == c, sc_s[...], pltpu.roll(sc_s[...], 32, 1)) for c in (0, 1)]
    for i in range(2):
        first = jnp.sum(jnp.where(lane == 0, scales[i], 0.0), axis=1, keepdims=True)
        a1_s[i:i + 1, :] = jnp.broadcast_to(first, (1, 128))

    def u_of_rows():
        for s in range(2):
            def body(b, accs):
                accs = list(accs)
                for j in range(4):
                    v = vb_s[j // 2, b, 8 * (j % 2):8 * (j % 2) + 8]
                    for t in range(tiles):
                        accs[t] = accs[t] + k_s[b, s, 8 * j:8 * j + 8, tile(t)] * v
                return tuple(accs)

            accs = lax.fori_loop(0, NZ, body, tuple(jnp.zeros((8, 128), f32) for _ in range(tiles)))
            for t in range(tiles):
                u_s[s, t:t + 1, :] = a_s[s, t:t + 1, :] / jnp.sum(accs[t], axis=0, keepdims=True)

    def start_columns(par):
        us = [[jnp.broadcast_to(u_s[s, t:t + 1, :], (8, 128)) for t in range(tiles)] for s in range(2)]

        def body(b, carry):
            for j in range(4):
                acc = [k_s[b, s, 8 * j:8 * j + 8, tile(t)] * us[s][t] for s in range(2) for t in range(tiles)]
                while len(acc) > 1:
                    acc = [p + q for p, q in zip(acc[::2], acc[1::2])]
                c_s[j // 2, b, 8 * (j % 2):8 * (j % 2) + 8] = acc[0]
            return carry

        lax.fori_loop(0, NZ, body, 0)
        slot = dbuf.at[par, core * (NDP // 2) + chip]
        slot[...] = jnp.concatenate([gather_rows(c_s[h].reshape(128, 128)) for h in range(2)], axis=0)
        send(slot, [dp_target(o) for o in DP_OFFSETS], dsend.at[par], drecv.at[par])

    def end_columns(par):
        wait(dbuf.at[par, 0:NDP - 1], dsend.at[par], drecv.at[par])
        c = [summed(dbuf, par, cloud * (NDP // 2), NDP // 2) * a1_s[i:i + 1] for i, cloud in enumerate((core, twin))]
        g = cube_root(k3_s[...] * ((v_s[0] * c[0]) * (v_s[1] * c[1])))
        for i in range(2):
            v_s[i] = g / c[i]
        return c, g

    def plain_step(step):
        par = lax.rem(step, 2)
        start_columns(par)
        end_columns(par)
        spread_all(vb_s, v_s[0])
        u_of_rows()

    def mirror(outer, carry):
        mpar = lax.rem(outer, 2)
        g = g_s[...]
        sq = [over_blocks(mpar, cloud, 16) * veff_s[i] for i, cloud in enumerate((core, twin))]
        cross = sq[0] * qs_s[1] + sq[1] * qs_s[0]
        prod = jnp.concatenate([mbuf[mpar, b, 0:16] * mbuf[mpar, NZ + b, 0:16] for b in range(NZ)], axis=0).T
        dots = jnp.concatenate([jnp.sum(prod[64 * h:64 * h + 64], axis=0, keepdims=True) for h in range(2)], axis=0)
        gg = -(cross - 2.0 * dots * (veff_s[0] * veff_s[1])) / (g * g)
        hh = sq[1] / g

        def mean(p):
            return jnp.sum(jnp.sum(p, axis=1, keepdims=True), axis=0, keepdims=True) / RANK

        k3_s[...] = g * jnp.exp(-STEP * (gg - mean(gg)))
        spread_all(fb_s, veff_s[1] * (2.0 * STEP * LOG2E) / g)
        spread_all(sb_s, (hh - mean(hh)) * (-STEP * LOG2E))
        spread_all(vb_s, veff_s[0])
        for b in range(NZ):
            m = mbuf[mpar, twin * NZ + b, 0:16]
            turned = pltpu.roll(m, 64, 1)
            for h, pair_of in ((0, jnp.where(lane < 64, m, turned)), (1, jnp.where(lane < 64, turned, m))):
                high, low = split(pair_of * fb_s[h, b])
                w4_s[32 * b + 16 * h:32 * b + 16 * h + 16, 0:128] = high
                w4_s[32 * b + 16 * h:32 * b + 16 * h + 16, 128:256] = low
        for s in range(2):
            for t in range(tiles // 2):
                cols = slice(t * 256, (t + 1) * 256)
                f = jnp.dot(w4_s[...], x4_s[s, :, cols], preferred_element_type=f32)
                ua = jnp.concatenate(
                    [jnp.broadcast_to(u_s[s, 2 * t + i:2 * t + i + 1, :], (16, 128)) for i in range(2)], axis=1
                )
                acc = jnp.zeros((8, 256), f32)
                for b in range(NZ):
                    for h in range(2):
                        rows = slice(16 * h, 16 * h + 16)
                        sh = sb_s[h, b]
                        q = vb_s[h, b]
                        e = jnp.exp2(f[32 * b + 16 * h:32 * b + 16 * h + 16] + jnp.concatenate([sh, sh], axis=1))
                        new = k_s[b, s, rows, cols] * ua * jnp.concatenate([q, q], axis=1) * e
                        k_s[b, s, rows, cols] = new
                        acc = acc + (new[0:8] + new[8:16])
                total = jnp.sum(acc, axis=0, keepdims=True)
                for i in range(2):
                    r = 2 * t + i
                    u_s[s, r:r + 1, :] = a_s[s, r:r + 1, :] / total[:, 128 * i:128 * i + 128]

        v_s[...] = jnp.ones((2, 2, 128), f32)

        @pl.when(outer == MIRROR - 1)
        def _():
            pair(4).start()

        base = outer * INNER

        def body(t, inner):
            plain_step(base + t)
            return inner

        lax.fori_loop(0, INNER - 1, body, 0)
        par = lax.rem(base + (INNER - 1), 2)
        npar = lax.rem(outer + 1, 2)

        @pl.when(outer < MIRROR - 1)
        def _():
            start_moments()

        @pl.when(outer == MIRROR - 1)
        def _():
            pair(5).start()

        start_columns(par)

        @pl.when(outer < MIRROR - 1)
        def _():
            middle_moments()

        @pl.when(outer == MIRROR - 1)
        def _():
            for t in range(tiles):
                ku_s[core, :, tile(t)] = k_s[z, core, :, tile(t)] * jnp.broadcast_to(u_s[core, t:t + 1, :], (32, 128))
            end_pair(4)
            end_pair(5)
            for t in range(tiles):
                ku_s[twin, :, tile(t)] = o_s[:, tile(t)] * jnp.broadcast_to(ou_s[t:t + 1, :], (32, 128))
            scaled().start()

        c, g = end_columns(par)
        g_s[...] = g
        for i in range(2):
            veff_s[i] = v_s[i] * a1_s[i:i + 1]
            qs_s[i] = c[i] * v_s[i]

        @pl.when(outer < MIRROR - 1)
        def _():
            end_moments(npar, ())
            wait(mbuf.at[npar, 0:2 * NZ - 1], msend.at[npar], mrecv.at[npar])

        return carry

    lax.fori_loop(0, MIRROR, mirror, 0)
    for i, cloud in ((0, core), (1, twin)):
        spread_all((vb_s, fb_s)[i], veff_s[i] * RANK)
        for h in range(2):
            vo_ref[cloud, 16 * h:16 * h + 16] = (vb_s, fb_s)[i][h, z]
    own = [
        pltpu.roll(jnp.broadcast_to(g_s[h:h + 1], (8, 128)), lax.rem(128 + 16 * h - z * 16, 128), 1)[0:1] for h in range(2)
    ]
    wo_ref[...] = jnp.where(lane < 16, own[0], own[1]) * (RANK / total_count)
    scaled().wait()


def finish(ku_ref, vo_ref, w_ref, lo_ref, ro_ref, wo_ref):
    for side, ref in ((0, lo_ref), (1, ro_ref)):
        for t in range(ref.shape[1] // 128):
            cols = slice(t * 128, (t + 1) * 128)
            ref[:, cols] = ku_ref[side, :, cols] * vo_ref[side]
    wo_ref[...] = w_ref[:, 0:wo_ref.shape[1]]


def shards(cloud_x, cloud_y, mass_x, mass_y, left_start, right_start, weight_start):
    ranks, points = left_start.shape
    total_count = float(points * lax.axis_size("dp"))
    tiles = points // 128
    f32 = jnp.float32
    bf16 = jnp.bfloat16
    dma = pltpu.SemaphoreType.DMA
    vmem = pl.BlockSpec(memory_space=pltpu.VMEM)
    scaled, scales, weights = pl.pallas_call(
        functools.partial(kernel, total_count),
        name="sinkhorn",
        out_shape=(
            jax.ShapeDtypeStruct((2, ranks, points), f32),
            jax.ShapeDtypeStruct((2, ranks, 128), f32),
            jax.ShapeDtypeStruct((1, 128), f32),
        ),
        in_specs=[pl.BlockSpec(memory_space=pl.ANY)] * 7,
        out_specs=[pl.BlockSpec(memory_space=pl.ANY), vmem, vmem],
        scratch_shapes=[
            pltpu.VMEM((1, ranks), f32),
            pltpu.VMEM((2, ranks, points), f32),
            pltpu.VMEM((2, 64, points), f32),
            pltpu.VMEM((2, tiles, 128), f32),
            pltpu.VMEM((NZ, 2, ranks, points), f32),
            pltpu.VMEM((2, 64, points), f32),
            pltpu.VMEM((2, 256, points), bf16),
            pltpu.VMEM((256, 256), bf16),
            pltpu.VMEM((2, tiles, 128), f32),
            pltpu.VMEM((2 * tiles, 128), f32),
            pltpu.VMEM((2, tiles, 128), f32),
            pltpu.VMEM((2, tiles, 128), f32),
            pltpu.VMEM((2, tiles, 128), f32),
            pltpu.VMEM((64, points), bf16),
            pltpu.VMEM((2, NZ, 16, 128), f32),
            pltpu.VMEM((64, 128), f32),
            pltpu.VMEM((2, NZ, 16, 128), f32),
            pltpu.VMEM((2, NZ, 16, 128), f32),
            pltpu.VMEM((2, NZ, 16, 128), f32),
            pltpu.VMEM((ranks, points), f32),
            pltpu.VMEM((tiles, 128), f32),
            pltpu.VMEM((2, ranks, points), f32),
            pltpu.VMEM((1, 128), f32),
            pltpu.VMEM((1, 128), f32),
            pltpu.VMEM((1, 128), f32),
            pltpu.VMEM((2, 2, 128), f32),
            pltpu.VMEM((2, 128), f32),
            pltpu.VMEM((2, 128), f32),
            pltpu.VMEM((2, 2, 128), f32),
            pltpu.VMEM((2, 2, 128), f32),
            pltpu.VMEM((2, NZ, 2 * tiles, 128), f32),
            pltpu.VMEM((2, NDP, 1, 128), f32),
            pltpu.VMEM((2, NDP, 2, 128), f32),
            pltpu.VMEM((NX, 24, 128), f32),
            pltpu.VMEM((NY, 24, 128), f32),
            pltpu.VMEM((2, 2 * NZ, 24, 128), f32),
            dma((2,)), dma((2,)), dma((2,)), dma((2,)), dma((2,)), dma((2,)),
            dma, dma, dma, dma, dma((2,)), dma((2,)),
            dma((NZ - 1, 2)), dma((NZ - 1, 2)), dma((6,)), dma((6,)), dma((8,)),
        ],
        compiler_params=pltpu.CompilerParams(collective_id=0, has_side_effects=True),
    )(
        cloud_x, cloud_y, mass_x.reshape(tiles, 128), mass_y.reshape(tiles, 128),
        left_start, right_start, weight_start[None],
    )
    left, right, weights = pl.pallas_call(
        finish,
        name="finish",
        out_shape=(
            jax.ShapeDtypeStruct((ranks, points), f32),
            jax.ShapeDtypeStruct((ranks, points), f32),
            jax.ShapeDtypeStruct((1, ranks), f32),
        ),
        in_specs=[vmem] * 3,
        out_specs=[vmem] * 3,
    )(scaled, scales, weights)
    return left, right, weights.reshape(ranks)


def solution(mesh):
    in_specs = (
        P(None, "dp"),
        P(None, "dp"),
        P("dp"),
        P("dp"),
        P("rank", "dp"),
        P("rank", "dp"),
        P("rank"),
    )
    out_specs = (P("rank", "dp"), P("rank", "dp"), P("rank"))
    return jax.shard_map(shards, mesh=mesh, in_specs=in_specs, out_specs=out_specs, check_vma=False)
```

```python
import functools

import jax
import jax.numpy as jnp
from jax import lax
from jax.experimental import pallas as pl
from jax.experimental.pallas import tpu as pltpu
from jax.sharding import PartitionSpec as P

RANK = 256
INNER = 4
MIRROR = 3
STEP = 2.0
MESH = pl.DeviceIdType.MESH
LOG2E = 1.4426950408889634

NX, NY, NC, NZ = 4, 8, 2, 8
NDP = NX * NY * NC


def far_first(n):
    return sorted(range(n), key=lambda d: -min(d, n - d))


DP_OFFSETS = sorted(
    [(dx, dy, dc) for dx in range(NX) for dy in range(NY) for dc in range(NC) if (dx, dy, dc) != (0, 0, 0)],
    key=lambda o: -(min(o[0], NX - o[0]) + min(o[1], NY - o[1])),
)
X_OFFSETS = [o for o in DP_OFFSETS if o[1] == 0 and o[2] == 0]
Y_OFFSETS = [o for o in DP_OFFSETS if o[0] == 0 and o[2] == 0]
Z_OFFSETS = [d for d in far_first(NZ) if d]


def cube_root(x):
    y = jnp.exp2(jnp.log2(x) * (1.0 / 3.0))
    y = y - (y - x / (y * y)) * (1.0 / 3.0)
    return jnp.where(x > 0.0, y, 0.0)


def split(x):
    high = x.astype(jnp.bfloat16)
    return high, (x - high.astype(jnp.float32)).astype(jnp.bfloat16)


def kernel(
    total_count,
    x_ref, y_ref, mx_ref, my_ref, left_ref, right_ref, w_ref,
    ku_ref, vo_ref, wo_ref,
    w_s, f_s, cl_s, m_s, k_s, cm_s, x4_s, w4_s, a_s, a1_s, n2_s, u_s, u1_s, uk_s, c_s, vb1_s, vb_s, fb_s, sb_s, o_s, ou_s, ku_s,
    v1_s, k1_s, sc_s, v_s, k3_s, g_s, veff_s, qs_s,
    zbuf, cbuf, dbuf, xbuf, ybuf, mbuf,
    zsend, zrecv, csend, crecv, dsend, drecv, xsend, xrecv, ysend, yrecv, msend, mrecv, asend, arecv, psend, precv, isem,
):
    dp = lax.axis_index("dp")
    z = lax.axis_index("rank")
    core = lax.rem(dp, NC)
    twin = 1 - core
    yy = lax.rem(lax.div(dp, NC), NY)
    xx = lax.div(dp, NC * NY)
    chip = lax.div(dp, NC)
    tiles = mx_ref.shape[0]
    f32 = jnp.float32

    def dp_target(o):
        tx = lax.rem(xx + o[0], NX)
        ty = lax.rem(yy + o[1], NY)
        tc = lax.rem(core + o[2], NC)
        return ((tx * NY + ty) * NC + tc, z)

    def z_target(d):
        return (dp, lax.rem(z + d, NZ))

    def zc_target(d):
        return (chip * NC + twin, lax.rem(z + d, NZ))

    partner = (chip * NC + twin, z)
    z_targets = [z_target(d) for d in Z_OFFSETS]
    zc_targets = [t(d) for d in Z_OFFSETS for t in (zc_target, z_target)] + [partner]

    barrier = pltpu.get_barrier_semaphore()
    for d in Z_OFFSETS:
        pl.semaphore_signal(barrier, inc=1, device_id=z_target(d), device_id_type=MESH)
        pl.semaphore_signal(barrier, inc=1, device_id=zc_target(d), device_id_type=MESH)
    for o in DP_OFFSETS:
        pl.semaphore_signal(barrier, inc=1, device_id=dp_target(o), device_id_type=MESH)

    def send(slot, targets, ssem, rsem):
        for t in targets:
            pltpu.make_async_remote_copy(
                src_ref=slot, dst_ref=slot, send_sem=ssem, recv_sem=rsem, device_id=t, device_id_type=MESH
            ).start()

    def wait(some, ssem, rsem):
        pltpu.make_async_copy(some, some, rsem).wait()
        pltpu.make_async_copy(some, some, ssem).wait()

    def pair(i):
        src, dst = (
            (f_s.at[twin], k_s.at[z, core]),
            (m_s.at[twin], a_s.at[core]),
            (cl_s.at[twin], cm_s.at[core]),
            (u1_s.at[twin], u_s.at[core]),
            (k_s.at[z, twin], o_s),
            (u_s.at[twin], ou_s),
        )[i]
        return pltpu.make_async_remote_copy(
            src_ref=src, dst_ref=dst, send_sem=psend.at[i], recv_sem=precv.at[i], device_id=partner, device_id_type=MESH
        )

    def scaled():
        return pltpu.make_async_copy(ku_s, ku_ref, isem.at[7])

    def end_pair(i):
        pair(i).wait_recv()
        pair(i).wait_send()

    def tile(t):
        return slice(t * 128, (t + 1) * 128)

    inputs = [
        pltpu.make_async_copy(src, dst, isem.at[i])
        for i, (src, dst) in enumerate((
            (left_ref, f_s.at[0]), (right_ref, f_s.at[1]), (mx_ref, m_s.at[0]), (my_ref, m_s.at[1]),
            (x_ref, cl_s.at[0]), (y_ref, cl_s.at[1]), (w_ref, w_s),
        ))
    ]
    for copy in inputs:
        copy.start()
    lane = lax.broadcasted_iota(jnp.int32, (1, 128), 1)
    for copy in inputs:
        copy.wait()
    a1_s[0:tiles, :] = m_s[0]
    a1_s[tiles:2 * tiles, :] = m_s[1]
    k_s[z, core] = f_s[core]
    a_s[core] = m_s[core]
    cm_s[core] = cl_s[core]
    k1_s[0:1, 0:w_s.shape[1]] = w_s[...]
    start = jnp.where(lane < 32, k1_s[...], 0.0)
    start = start + pltpu.roll(start, 32, 1)
    k1_s[...] = start + pltpu.roll(start, 64, 1)
    pl.semaphore_wait(barrier, 2 * len(Z_OFFSETS) + len(DP_OFFSETS))
    for i in range(3):
        pair(i).start()

    def spread(vec):
        return jnp.broadcast_to(vec, (128, 128)).T

    def spread_all(dst, vec):
        for h in range(2):
            dst[h] = spread(vec[h:h + 1]).reshape(NZ, 16, 128)

    def gather_rows(rows):
        return jnp.sum(rows.T, axis=0, keepdims=True)

    def swap(p):
        return jnp.where(lax.rem(lane, 64) < 32, pltpu.roll(p, 96, 1), pltpu.roll(p, 32, 1))

    def doubled(c):
        return jnp.where(lane < 64, c, pltpu.roll(c, 64, 1))

    def ring_copies(i):
        hop, late = divmod(i, 2)
        copies = []
        for way, sign in ((0, 1), (1, -1)):
            part = k_s.at[lax.rem(z - sign * hop + NZ, NZ), (way + late) % 2]
            copies.append(pltpu.make_async_remote_copy(
                src_ref=part, dst_ref=part, send_sem=asend.at[i, way], recv_sem=arecv.at[i, way],
                device_id=(dp, lax.rem(z + sign + NZ, NZ)), device_id_type=MESH,
            ))
        return copies

    def ring_end(i):
        for copy in ring_copies(i):
            copy.wait_recv()
            copy.wait_send()

    def ring(i):
        if i >= 2:
            ring_end(i - 2)
        for copy in ring_copies(i):
            copy.start()

    def at(step, when, action):
        @pl.when(step == when)
        def _():
            action()

    def row_sums(step):
        par = lax.rem(step, 2)
        for t in range(tiles):
            for side in range(2):
                i = side * tiles + t
                b = f_s[side, :, tile(t)] * vb1_s[32 * side:32 * side + 32]
                zbuf[par, z, i:i + 1, :] = jnp.sum(b, axis=0, keepdims=True)
        send(zbuf.at[par, z], z_targets, zsend.at[par], zrecv.at[par])

        def first():
            end_pair(0)
            ring(0)
            end_pair(1)
            end_pair(2)
            prepare()

        at(step, 0, first)
        at(step, 2, lambda: ring(3))
        at(step, 3, lambda: ring(5))
        wait(zbuf.at[par, 0:NZ - 1], zsend.at[par], zrecv.at[par])
        total = zbuf[par, 0]
        for i in range(1, NZ):
            total = total + zbuf[par, i]
        u = a1_s[...] / total
        u1_s[0] = u[0:tiles]
        u1_s[1] = u[tiles:2 * tiles]

    def prepare():
        for s in range(2):
            for t in range(tiles):
                b = cm_s[s, :, tile(t)]
                n2_s[s, t:t + 1, :] = jnp.sum(b * b, axis=0, keepdims=True)
                high, low = split(b)
                both = jnp.concatenate([high, low], axis=0)
                x4_s[s, 0:128, tile(t)] = both
                x4_s[s, 128:256, tile(t)] = both

    def own_columns():
        accs = []
        for side in range(2):
            acc = jnp.zeros((32, 128), f32)
            for t in range(tiles):
                acc = acc + f_s[side, :, tile(t)] * jnp.broadcast_to(u1_s[side, t:t + 1, :], (32, 128))
            accs.append(acc)
        return accs

    def summed(buf, par, first, count):
        parts = [buf[par, first + i] for i in range(4)]
        for i in range(4, count):
            parts[i % 4] = parts[i % 4] + buf[par, first + i]
        return (parts[0] + parts[1]) + (parts[2] + parts[3])

    def exchange_first(par, low, high):
        cbuf[par, dp] = gather_rows(jnp.concatenate(low + high, axis=0))
        send(cbuf.at[par, dp], [dp_target(o) for o in DP_OFFSETS], csend.at[par], crecv.at[par])

    def rescale_first(c):
        v = v1_s[...]
        p = v * c
        g = cube_root(k1_s[...] * (p * swap(p)))
        v = g / c
        v1_s[...] = v
        return g, v

    def first_step(step, carry):
        par = lax.rem(step, 2)
        row_sums(step)
        ax = jnp.sum(a1_s[0:tiles, :], axis=0, keepdims=True)
        ay = jnp.sum(a1_s[tiles:2 * tiles, :], axis=0, keepdims=True)
        exchange_first(par, own_columns(), [jnp.broadcast_to(ax, (32, 128)), jnp.broadcast_to(ay, (32, 128))])
        at(step, 0, lambda: ring(1))
        at(step, 1, lambda: ring(2))
        at(step, 2, lambda: ring(4))
        wait(cbuf.at[par, 0:NDP - 1], csend.at[par], crecv.at[par])
        c = summed(cbuf, par, 0, NDP)
        scale = total_count / jnp.where(lane >= 64, c, pltpu.roll(c, 64, 1))
        sc_s[...] = scale
        g, v = rescale_first(doubled(c) * scale)
        vb1_s[...] = spread(v)[0:64]
        return carry

    def placed(row, offset):
        moved = pltpu.roll(jnp.broadcast_to(row, (8, 128)), lax.rem(z * 16 - offset + 256, 128), 1)[0:1]
        return jnp.where((lane >= z * 16) & (lane < z * 16 + 16), moved, 0.0)

    def start_moments():
        acc = jnp.zeros((32, 128), f32)
        both = jnp.zeros((32, 128), f32)
        for s in range(2):
            for t in range(tiles):
                b = k_s[z, s, :, tile(t)] * jnp.broadcast_to(u_s[s, t:t + 1, :], (32, 128))
                acc = acc + b * jnp.broadcast_to(n2_s[s, t:t + 1, :], (32, 128))
                high, low = split(b)
                uk_s[s, 0:32, tile(t)] = high
                uk_s[s, 32:64, tile(t)] = low
            d = lax.dot_general(
                uk_s[s], x4_s[s, 0:128, :], (((1,), (1,)), ((), ())), preferred_element_type=f32
            )
            both = both + d[0:32] + d[32:64]
        both = both + pltpu.roll(both, 64, 1)
        xbuf[xx, 0:16] = jnp.where(lane < 64, both[0:16], both[16:32])
        sums = gather_rows(jnp.concatenate([acc] * 4, axis=0))
        xbuf[xx, 16:17] = placed(sums, 0)
        xbuf[xx, 17:18] = placed(sums, 16)
        send(xbuf.at[xx], [dp_target(o) for o in X_OFFSETS], xsend, xrecv)

    def middle_moments():
        wait(xbuf.at[0:NX - 1], xsend, xrecv)
        m = xbuf[0]
        for i in range(1, NX):
            m = m + xbuf[i]
        ybuf[yy] = m
        send(ybuf.at[yy], [dp_target(o) for o in Y_OFFSETS], ysend, yrecv)

    def end_moments(par, rows):
        wait(ybuf.at[0:NY - 1], ysend, yrecv)
        m = ybuf[0]
        for i in range(1, NY):
            m = m + ybuf[i]
        mbuf[par, core * NZ + z, 0:18] = m
        for i, row in enumerate(rows):
            mbuf[par, core * NZ + z, 18 + i:19 + i] = row
        send(mbuf.at[par, core * NZ + z, 0:18 + len(rows)], zc_targets, msend.at[par], mrecv.at[par])

    v1_s[...] = jnp.ones((1, 128), f32)
    vb1_s[...] = jnp.ones((64, 128), f32)
    lax.fori_loop(0, INNER - 1, first_step, 0)
    par = (INNER - 1) % 2
    row_sums(jnp.int32(INNER - 1))
    pair(3).start()
    u_s[core] = u1_s[core]
    accs = own_columns()
    exchange_first(par, accs, accs)
    end_pair(3)
    start_moments()
    ring(6)
    middle_moments()
    wait(cbuf.at[par, 0:NDP - 1], csend.at[par], crecv.at[par])
    c1 = summed(cbuf, par, 0, NDP) * sc_s[...]
    g1, v1 = rescale_first(c1)
    mine = core * 32
    e1 = v1 * sc_s[...]
    q1 = c1 * v1
    end_moments(0, [placed(p, mine + 16 * h) for p in (g1, e1, q1) for h in range(2)])
    ring_end(5)
    ring_end(6)
    wait(mbuf.at[0, 0:2 * NZ - 1], msend.at[0], mrecv.at[0])

    def over_blocks(par, cloud, first):
        rows = mbuf[par, cloud * NZ, first:first + 2]
        for b in range(1, NZ):
            rows = rows + mbuf[par, cloud * NZ + b, first:first + 2]
        return rows

    g_s[...] = over_blocks(0, core, 18)
    for i, cloud in enumerate((core, twin)):
        veff_s[i] = over_blocks(0, cloud, 20)
        qs_s[i] = over_blocks(0, cloud, 22)
    scales = [jnp.where(core == c, sc_s[...], pltpu.roll(sc_s[...], 32, 1)) for c in (0, 1)]
    for i in range(2):
        first = jnp.sum(jnp.where(lane == 0, scales[i], 0.0), axis=1, keepdims=True)
        a1_s[i:i + 1, :] = jnp.broadcast_to(first, (1, 128))

    def u_of_rows():
        for s in range(2):
            def body(b, accs):
                accs = list(accs)
                for j in range(4):
                    v = vb_s[j // 2, b, 8 * (j % 2):8 * (j % 2) + 8]
                    for t in range(tiles):
                        accs[t] = accs[t] + k_s[b, s, 8 * j:8 * j + 8, tile(t)] * v
                return tuple(accs)

            accs = lax.fori_loop(0, NZ, body, tuple(jnp.zeros((8, 128), f32) for _ in range(tiles)), unroll=True)
            for t in range(tiles):
                u_s[s, t:t + 1, :] = a_s[s, t:t + 1, :] / jnp.sum(accs[t], axis=0, keepdims=True)

    def start_columns(par):
        us = [[jnp.broadcast_to(u_s[s, t:t + 1, :], (8, 128)) for t in range(tiles)] for s in range(2)]

        def body(b, carry):
            for j in range(4):
                acc = [k_s[b, s, 8 * j:8 * j + 8, tile(t)] * us[s][t] for s in range(2) for t in range(tiles)]
                while len(acc) > 1:
                    acc = [p + q for p, q in zip(acc[::2], acc[1::2])]
                c_s[j // 2, b, 8 * (j % 2):8 * (j % 2) + 8] = acc[0]
            return carry

        lax.fori_loop(0, NZ, body, 0, unroll=True)
        slot = dbuf.at[par, core * (NDP // 2) + chip]
        slot[...] = jnp.concatenate([gather_rows(c_s[h].reshape(128, 128)) for h in range(2)], axis=0)
        send(slot, [dp_target(o) for o in DP_OFFSETS], dsend.at[par], drecv.at[par])

    def end_columns(par):
        wait(dbuf.at[par, 0:NDP - 1], dsend.at[par], drecv.at[par])
        c = [summed(dbuf, par, cloud * (NDP // 2), NDP // 2) * a1_s[i:i + 1] for i, cloud in enumerate((core, twin))]
        g = cube_root(k3_s[...] * ((v_s[0] * c[0]) * (v_s[1] * c[1])))
        for i in range(2):
            v_s[i] = g / c[i]
        return c, g

    def plain_step(step):
        par = lax.rem(step, 2)
        start_columns(par)
        end_columns(par)
        spread_all(vb_s, v_s[0])
        u_of_rows()

    def mirror(outer, carry):
        mpar = lax.rem(outer, 2)
        g = g_s[...]
        sq = [over_blocks(mpar, cloud, 16) * veff_s[i] for i, cloud in enumerate((core, twin))]
        cross = sq[0] * qs_s[1] + sq[1] * qs_s[0]
        prod = jnp.concatenate([mbuf[mpar, b, 0:16] * mbuf[mpar, NZ + b, 0:16] for b in range(NZ)], axis=0).T
        dots = jnp.concatenate([jnp.sum(prod[64 * h:64 * h + 64], axis=0, keepdims=True) for h in range(2)], axis=0)
        gg = -(cross - 2.0 * dots * (veff_s[0] * veff_s[1])) / (g * g)
        hh = sq[1] / g

        def mean(p):
            return jnp.sum(jnp.sum(p, axis=1, keepdims=True), axis=0, keepdims=True) / RANK

        k3_s[...] = g * jnp.exp(-STEP * (gg - mean(gg)))
        spread_all(fb_s, veff_s[1] * (2.0 * STEP * LOG2E) / g)
        spread_all(sb_s, (hh - mean(hh)) * (-STEP * LOG2E))
        spread_all(vb_s, veff_s[0])
        for b in range(NZ):
            m = mbuf[mpar, twin * NZ + b, 0:16]
            turned = pltpu.roll(m, 64, 1)
            for h, pair_of in ((0, jnp.where(lane < 64, m, turned)), (1, jnp.where(lane < 64, turned, m))):
                high, low = split(pair_of * fb_s[h, b])
                w4_s[32 * b + 16 * h:32 * b + 16 * h + 16, 0:128] = high
                w4_s[32 * b + 16 * h:32 * b + 16 * h + 16, 128:256] = low
        for s in range(2):
            for t in range(tiles // 2):
                cols = slice(t * 256, (t + 1) * 256)
                f = jnp.dot(w4_s[...], x4_s[s, :, cols], preferred_element_type=f32)
                ua = jnp.concatenate(
                    [jnp.broadcast_to(u_s[s, 2 * t + i:2 * t + i + 1, :], (16, 128)) for i in range(2)], axis=1
                )
                acc = jnp.zeros((8, 256), f32)
                for b in range(NZ):
                    for h in range(2):
                        rows = slice(16 * h, 16 * h + 16)
                        sh = sb_s[h, b]
                        q = vb_s[h, b]
                        e = jnp.exp2(f[32 * b + 16 * h:32 * b + 16 * h + 16] + jnp.concatenate([sh, sh], axis=1))
                        new = k_s[b, s, rows, cols] * ua * jnp.concatenate([q, q], axis=1) * e
                        k_s[b, s, rows, cols] = new
                        acc = acc + (new[0:8] + new[8:16])
                total = jnp.sum(acc, axis=0, keepdims=True)
                for i in range(2):
                    r = 2 * t + i
                    u_s[s, r:r + 1, :] = a_s[s, r:r + 1, :] / total[:, 128 * i:128 * i + 128]

        v_s[...] = jnp.ones((2, 2, 128), f32)

        @pl.when(outer == MIRROR - 1)
        def _():
            pair(4).start()

        base = outer * INNER

        def body(t, inner):
            plain_step(base + t)
            return inner

        lax.fori_loop(0, INNER - 1, body, 0)
        par = lax.rem(base + (INNER - 1), 2)
        npar = lax.rem(outer + 1, 2)

        @pl.when(outer < MIRROR - 1)
        def _():
            start_moments()

        @pl.when(outer == MIRROR - 1)
        def _():
            pair(5).start()

        start_columns(par)

        @pl.when(outer < MIRROR - 1)
        def _():
            middle_moments()

        @pl.when(outer == MIRROR - 1)
        def _():
            for t in range(tiles):
                ku_s[core, :, tile(t)] = k_s[z, core, :, tile(t)] * jnp.broadcast_to(u_s[core, t:t + 1, :], (32, 128))
            end_pair(4)
            end_pair(5)
            for t in range(tiles):
                ku_s[twin, :, tile(t)] = o_s[:, tile(t)] * jnp.broadcast_to(ou_s[t:t + 1, :], (32, 128))
            scaled().start()

        c, g = end_columns(par)
        g_s[...] = g
        for i in range(2):
            veff_s[i] = v_s[i] * a1_s[i:i + 1]
            qs_s[i] = c[i] * v_s[i]

        @pl.when(outer < MIRROR - 1)
        def _():
            end_moments(npar, ())
            wait(mbuf.at[npar, 0:2 * NZ - 1, 0:18], msend.at[npar], mrecv.at[npar])

        return carry

    lax.fori_loop(0, MIRROR, mirror, 0)
    for i, cloud in ((0, core), (1, twin)):
        spread_all((vb_s, fb_s)[i], veff_s[i] * RANK)
        for h in range(2):
            vo_ref[cloud, 16 * h:16 * h + 16] = (vb_s, fb_s)[i][h, z]
    own = [
        pltpu.roll(jnp.broadcast_to(g_s[h:h + 1], (8, 128)), lax.rem(128 + 16 * h - z * 16, 128), 1)[0:1] for h in range(2)
    ]
    wo_ref[...] = jnp.where(lane < 16, own[0], own[1]) * (RANK / total_count)
    scaled().wait()


def finish(ku_ref, vo_ref, w_ref, lo_ref, ro_ref, wo_ref):
    for side, ref in ((0, lo_ref), (1, ro_ref)):
        for t in range(ref.shape[1] // 128):
            cols = slice(t * 128, (t + 1) * 128)
            ref[:, cols] = ku_ref[side, :, cols] * vo_ref[side]
    wo_ref[...] = w_ref[:, 0:wo_ref.shape[1]]


def shards(cloud_x, cloud_y, mass_x, mass_y, left_start, right_start, weight_start):
    ranks, points = left_start.shape
    total_count = float(points * lax.axis_size("dp"))
    tiles = points // 128
    f32 = jnp.float32
    bf16 = jnp.bfloat16
    dma = pltpu.SemaphoreType.DMA
    vmem = pl.BlockSpec(memory_space=pltpu.VMEM)
    scaled, scales, weights = pl.pallas_call(
        functools.partial(kernel, total_count),
        name="sinkhorn",
        out_shape=(
            jax.ShapeDtypeStruct((2, ranks, points), f32),
            jax.ShapeDtypeStruct((2, ranks, 128), f32),
            jax.ShapeDtypeStruct((1, 128), f32),
        ),
        in_specs=[pl.BlockSpec(memory_space=pl.ANY)] * 7,
        out_specs=[pl.BlockSpec(memory_space=pl.ANY), vmem, vmem],
        scratch_shapes=[
            pltpu.VMEM((1, ranks), f32),
            pltpu.VMEM((2, ranks, points), f32),
            pltpu.VMEM((2, 64, points), f32),
            pltpu.VMEM((2, tiles, 128), f32),
            pltpu.VMEM((NZ, 2, ranks, points), f32),
            pltpu.VMEM((2, 64, points), f32),
            pltpu.VMEM((2, 256, points), bf16),
            pltpu.VMEM((256, 256), bf16),
            pltpu.VMEM((2, tiles, 128), f32),
            pltpu.VMEM((2 * tiles, 128), f32),
            pltpu.VMEM((2, tiles, 128), f32),
            pltpu.VMEM((2, tiles, 128), f32),
            pltpu.VMEM((2, tiles, 128), f32),
            pltpu.VMEM((2, 64, points), bf16),
            pltpu.VMEM((2, NZ, 16, 128), f32),
            pltpu.VMEM((64, 128), f32),
            pltpu.VMEM((2, NZ, 16, 128), f32),
            pltpu.VMEM((2, NZ, 16, 128), f32),
            pltpu.VMEM((2, NZ, 16, 128), f32),
            pltpu.VMEM((ranks, points), f32),
            pltpu.VMEM((tiles, 128), f32),
            pltpu.VMEM((2, ranks, points), f32),
            pltpu.VMEM((1, 128), f32),
            pltpu.VMEM((1, 128), f32),
            pltpu.VMEM((1, 128), f32),
            pltpu.VMEM((2, 2, 128), f32),
            pltpu.VMEM((2, 128), f32),
            pltpu.VMEM((2, 128), f32),
            pltpu.VMEM((2, 2, 128), f32),
            pltpu.VMEM((2, 2, 128), f32),
            pltpu.VMEM((2, NZ, 2 * tiles, 128), f32),
            pltpu.VMEM((2, NDP, 1, 128), f32),
            pltpu.VMEM((2, NDP, 2, 128), f32),
            pltpu.VMEM((NX, 18, 128), f32),
            pltpu.VMEM((NY, 18, 128), f32),
            pltpu.VMEM((2, 2 * NZ, 24, 128), f32),
            dma((2,)), dma((2,)), dma((2,)), dma((2,)), dma((2,)), dma((2,)),
            dma, dma, dma, dma, dma((2,)), dma((2,)),
            dma((NZ - 1, 2)), dma((NZ - 1, 2)), dma((6,)), dma((6,)), dma((8,)),
        ],
        compiler_params=pltpu.CompilerParams(collective_id=0, has_side_effects=True),
    )(
        cloud_x, cloud_y, mass_x.reshape(tiles, 128), mass_y.reshape(tiles, 128),
        left_start, right_start, weight_start[None],
    )
    left, right, weights = pl.pallas_call(
        finish,
        name="finish",
        out_shape=(
            jax.ShapeDtypeStruct((ranks, points), f32),
            jax.ShapeDtypeStruct((ranks, points), f32),
            jax.ShapeDtypeStruct((1, ranks), f32),
        ),
        in_specs=[vmem] * 3,
        out_specs=[vmem] * 3,
    )(scaled, scales, weights)
    return left, right, weights.reshape(ranks)


def solution(mesh):
    in_specs = (
        P(None, "dp"),
        P(None, "dp"),
        P("dp"),
        P("dp"),
        P("rank", "dp"),
        P("rank", "dp"),
        P("rank"),
    )
    out_specs = (P("rank", "dp"), P("rank", "dp"), P("rank"))
    return jax.shard_map(shards, mesh=mesh, in_specs=in_specs, out_specs=out_specs, check_vma=False)
```

```python
import functools

import jax
import jax.numpy as jnp
from jax import lax
from jax.experimental import pallas as pl
from jax.experimental.pallas import tpu as pltpu
from jax.sharding import PartitionSpec as P

RANK = 256
INNER = 4
MIRROR = 3
STEP = 2.0
MESH = pl.DeviceIdType.MESH
LOG2E = 1.4426950408889634

NX, NY, NC, NZ = 4, 8, 2, 8
NDP = NX * NY * NC


def far_first(n):
    return sorted(range(n), key=lambda d: -min(d, n - d))


DP_OFFSETS = sorted(
    [(dx, dy, dc) for dx in range(NX) for dy in range(NY) for dc in range(NC) if (dx, dy, dc) != (0, 0, 0)],
    key=lambda o: -(min(o[0], NX - o[0]) + min(o[1], NY - o[1])),
)
X_OFFSETS = [o for o in DP_OFFSETS if o[1] == 0 and o[2] == 0]
Y_OFFSETS = [o for o in DP_OFFSETS if o[0] == 0 and o[2] == 0]
Z_OFFSETS = [d for d in far_first(NZ) if d]


def cube_root(x):
    y = jnp.exp2(jnp.log2(x) * (1.0 / 3.0))
    y = y - (y - x / (y * y)) * (1.0 / 3.0)
    return jnp.where(x > 0.0, y, 0.0)


def split(x):
    high = x.astype(jnp.bfloat16)
    return high, (x - high.astype(jnp.float32)).astype(jnp.bfloat16)


def kernel(
    total_count,
    x_ref, y_ref, mx_ref, my_ref, left_ref, right_ref, w_ref,
    ku_ref, vo_ref, wo_ref,
    w_s, f_s, cl_s, m_s, k_s, cm_s, x4_s, w4_s, a_s, a1_s, n2_s, u_s, u1_s, uk_s, c_s, vb1_s, vb_s, fb_s, sb_s, o_s, ou_s, ku_s,
    v1_s, k1_s, sc_s, v_s, k3_s, g_s, veff_s, qs_s,
    zbuf, cbuf, dbuf, xbuf, ybuf, mbuf,
    zsend, zrecv, csend, crecv, dsend, drecv, xsend, xrecv, ysend, yrecv, msend, mrecv, asend, arecv, psend, precv, isem,
):
    dp = lax.axis_index("dp")
    z = lax.axis_index("rank")
    core = lax.rem(dp, NC)
    twin = 1 - core
    yy = lax.rem(lax.div(dp, NC), NY)
    xx = lax.div(dp, NC * NY)
    chip = lax.div(dp, NC)
    tiles = mx_ref.shape[0]
    f32 = jnp.float32

    def dp_target(o):
        tx = lax.rem(xx + o[0], NX)
        ty = lax.rem(yy + o[1], NY)
        tc = lax.rem(core + o[2], NC)
        return ((tx * NY + ty) * NC + tc, z)

    def z_target(d):
        return (dp, lax.rem(z + d, NZ))

    def zc_target(d):
        return (chip * NC + twin, lax.rem(z + d, NZ))

    partner = (chip * NC + twin, z)
    z_targets = [z_target(d) for d in Z_OFFSETS]
    zc_targets = [t(d) for d in Z_OFFSETS for t in (zc_target, z_target)] + [partner]

    inputs = [
        pltpu.make_async_copy(src, dst, isem.at[i])
        for i, (src, dst) in enumerate((
            (left_ref, f_s.at[0]), (right_ref, f_s.at[1]), (mx_ref, m_s.at[0]), (my_ref, m_s.at[1]),
            (x_ref, cl_s.at[0]), (y_ref, cl_s.at[1]), (w_ref, w_s),
        ))
    ]
    for copy in inputs:
        copy.start()
    barrier = pltpu.get_barrier_semaphore()
    for d in Z_OFFSETS:
        pl.semaphore_signal(barrier, inc=1, device_id=z_target(d), device_id_type=MESH)
        pl.semaphore_signal(barrier, inc=1, device_id=zc_target(d), device_id_type=MESH)
    for o in DP_OFFSETS:
        pl.semaphore_signal(barrier, inc=1, device_id=dp_target(o), device_id_type=MESH)

    def send(slot, targets, ssem, rsem):
        for t in targets:
            pltpu.make_async_remote_copy(
                src_ref=slot, dst_ref=slot, send_sem=ssem, recv_sem=rsem, device_id=t, device_id_type=MESH
            ).start()

    def wait(some, ssem, rsem):
        pltpu.make_async_copy(some, some, rsem).wait()
        pltpu.make_async_copy(some, some, ssem).wait()

    def pair(i):
        src, dst = (
            (f_s.at[twin], k_s.at[z, core]),
            (m_s.at[twin], a_s.at[core]),
            (cl_s.at[twin], cm_s.at[core]),
            (u1_s.at[twin], u_s.at[core]),
            (k_s.at[z, twin], o_s),
            (u_s.at[twin], ou_s),
        )[i]
        return pltpu.make_async_remote_copy(
            src_ref=src, dst_ref=dst, send_sem=psend.at[i], recv_sem=precv.at[i], device_id=partner, device_id_type=MESH
        )

    def scaled():
        return pltpu.make_async_copy(ku_s, ku_ref, isem.at[7])

    def end_pair(i):
        pair(i).wait_recv()
        pair(i).wait_send()

    def tile(t):
        return slice(t * 128, (t + 1) * 128)

    def own_rows(par):
        for t in range(tiles):
            for side in range(2):
                i = side * tiles + t
                b = f_s[side, :, tile(t)] * vb1_s[32 * side:32 * side + 32]
                zbuf[par, z, i:i + 1, :] = jnp.sum(b, axis=0, keepdims=True)

    lane = lax.broadcasted_iota(jnp.int32, (1, 128), 1)
    for copy in inputs:
        copy.wait()
    a1_s[0:tiles, :] = m_s[0]
    a1_s[tiles:2 * tiles, :] = m_s[1]
    k_s[z, core] = f_s[core]
    a_s[core] = m_s[core]
    cm_s[core] = cl_s[core]
    k1_s[0:1, 0:w_s.shape[1]] = w_s[...]
    start = jnp.where(lane < 32, k1_s[...], 0.0)
    start = start + pltpu.roll(start, 32, 1)
    k1_s[...] = start + pltpu.roll(start, 64, 1)
    v1_s[...] = jnp.ones((1, 128), f32)
    vb1_s[...] = jnp.ones((64, 128), f32)
    own_rows(0)
    pl.semaphore_wait(barrier, 2 * len(Z_OFFSETS) + len(DP_OFFSETS))
    for i in range(3):
        pair(i).start()

    def spread(vec):
        return jnp.broadcast_to(vec, (128, 128)).T

    def spread_all(dst, vec):
        for h in range(2):
            dst[h] = spread(vec[h:h + 1]).reshape(NZ, 16, 128)

    def gather_rows(rows):
        return jnp.sum(rows.T, axis=0, keepdims=True)

    def swap(p):
        return jnp.where(lax.rem(lane, 64) < 32, pltpu.roll(p, 96, 1), pltpu.roll(p, 32, 1))

    def doubled(c):
        return jnp.where(lane < 64, c, pltpu.roll(c, 64, 1))

    def ring_copies(i):
        hop, late = divmod(i, 2)
        copies = []
        for way, sign in ((0, 1), (1, -1)):
            part = k_s.at[lax.rem(z - sign * hop + NZ, NZ), (way + late) % 2]
            copies.append(pltpu.make_async_remote_copy(
                src_ref=part, dst_ref=part, send_sem=asend.at[i, way], recv_sem=arecv.at[i, way],
                device_id=(dp, lax.rem(z + sign + NZ, NZ)), device_id_type=MESH,
            ))
        return copies

    def ring_end(i):
        for copy in ring_copies(i):
            copy.wait_recv()
            copy.wait_send()

    def ring(i):
        if i >= 2:
            ring_end(i - 2)
        for copy in ring_copies(i):
            copy.start()

    def at(step, when, action):
        @pl.when(step == when)
        def _():
            action()

    def row_sums(step):
        par = lax.rem(step, 2)
        send(zbuf.at[par, z], z_targets, zsend.at[par], zrecv.at[par])

        def first():
            end_pair(0)
            ring(0)
            end_pair(1)
            end_pair(2)
            prepare()

        at(step, 0, first)
        at(step, 2, lambda: ring(3))
        at(step, 3, lambda: ring(5))
        wait(zbuf.at[par, 0:NZ - 1], zsend.at[par], zrecv.at[par])
        total = zbuf[par, 0]
        for i in range(1, NZ):
            total = total + zbuf[par, i]
        u = a1_s[...] / total
        u1_s[0] = u[0:tiles]
        u1_s[1] = u[tiles:2 * tiles]

    def prepare():
        for s in range(2):
            for t in range(tiles):
                b = cm_s[s, :, tile(t)]
                n2_s[s, t:t + 1, :] = jnp.sum(b * b, axis=0, keepdims=True)
                high, low = split(b)
                both = jnp.concatenate([high, low], axis=0)
                x4_s[s, 0:128, tile(t)] = both
                x4_s[s, 128:256, tile(t)] = both

    def own_columns():
        accs = []
        for side in range(2):
            acc = jnp.zeros((32, 128), f32)
            for t in range(tiles):
                acc = acc + f_s[side, :, tile(t)] * jnp.broadcast_to(u1_s[side, t:t + 1, :], (32, 128))
            accs.append(acc)
        return accs

    def summed(buf, par, first, count):
        parts = [buf[par, first + i] for i in range(4)]
        for i in range(4, count):
            parts[i % 4] = parts[i % 4] + buf[par, first + i]
        return (parts[0] + parts[1]) + (parts[2] + parts[3])

    def exchange_first(par, low, high):
        cbuf[par, dp] = gather_rows(jnp.concatenate(low + high, axis=0))
        send(cbuf.at[par, dp], [dp_target(o) for o in DP_OFFSETS], csend.at[par], crecv.at[par])

    def rescale_first(c):
        v = v1_s[...]
        p = v * c
        g = cube_root(k1_s[...] * (p * swap(p)))
        v = g / c
        v1_s[...] = v
        return g, v

    def first_step(step, carry):
        par = lax.rem(step, 2)
        row_sums(step)
        ax = jnp.sum(a1_s[0:tiles, :], axis=0, keepdims=True)
        ay = jnp.sum(a1_s[tiles:2 * tiles, :], axis=0, keepdims=True)
        exchange_first(par, own_columns(), [jnp.broadcast_to(ax, (32, 128)), jnp.broadcast_to(ay, (32, 128))])
        at(step, 0, lambda: ring(1))
        at(step, 1, lambda: ring(2))
        at(step, 2, lambda: ring(4))
        wait(cbuf.at[par, 0:NDP - 1], csend.at[par], crecv.at[par])
        c = summed(cbuf, par, 0, NDP)
        scale = total_count / jnp.where(lane >= 64, c, pltpu.roll(c, 64, 1))
        sc_s[...] = scale
        g, v = rescale_first(doubled(c) * scale)
        vb1_s[...] = spread(v)[0:64]
        own_rows(1 - par)
        return carry

    def placed(row, offset):
        moved = pltpu.roll(jnp.broadcast_to(row, (8, 128)), lax.rem(z * 16 - offset + 256, 128), 1)[0:1]
        return jnp.where((lane >= z * 16) & (lane < z * 16 + 16), moved, 0.0)

    def start_moments(between=None):
        acc = jnp.zeros((32, 128), f32)
        both = jnp.zeros((32, 128), f32)
        for i, s in enumerate((core, twin)):
            if i and between:
                between()
            for t in range(tiles):
                b = k_s[z, s, :, tile(t)] * jnp.broadcast_to(u_s[s, t:t + 1, :], (32, 128))
                acc = acc + b * jnp.broadcast_to(n2_s[s, t:t + 1, :], (32, 128))
                high, low = split(b)
                uk_s[i, 0:32, tile(t)] = high
                uk_s[i, 32:64, tile(t)] = low
            d = lax.dot_general(
                uk_s[i], x4_s[s, 0:128, :], (((1,), (1,)), ((), ())), preferred_element_type=f32
            )
            both = both + d[0:32] + d[32:64]
        both = both + pltpu.roll(both, 64, 1)
        xbuf[xx, 0:16] = jnp.where(lane < 64, both[0:16], both[16:32])
        sums = gather_rows(jnp.concatenate([acc] * 4, axis=0))
        xbuf[xx, 16:17] = placed(sums, 0)
        xbuf[xx, 17:18] = placed(sums, 16)
        send(xbuf.at[xx], [dp_target(o) for o in X_OFFSETS], xsend, xrecv)

    def middle_moments():
        wait(xbuf.at[0:NX - 1], xsend, xrecv)
        m = xbuf[0]
        for i in range(1, NX):
            m = m + xbuf[i]
        ybuf[yy] = m
        send(ybuf.at[yy], [dp_target(o) for o in Y_OFFSETS], ysend, yrecv)

    def end_moments(par, rows):
        wait(ybuf.at[0:NY - 1], ysend, yrecv)
        m = ybuf[0]
        for i in range(1, NY):
            m = m + ybuf[i]
        mbuf[par, core * NZ + z, 0:18] = m
        for i, row in enumerate(rows):
            mbuf[par, core * NZ + z, 18 + i:19 + i] = row
        send(mbuf.at[par, core * NZ + z, 0:18 + len(rows)], zc_targets, msend.at[par], mrecv.at[par])

    lax.fori_loop(0, INNER - 1, first_step, 0)
    par = (INNER - 1) % 2
    row_sums(jnp.int32(INNER - 1))
    pair(3).start()
    u_s[core] = u1_s[core]
    accs = own_columns()
    exchange_first(par, accs, accs)
    start_moments(lambda: end_pair(3))
    ring(6)
    middle_moments()
    wait(cbuf.at[par, 0:NDP - 1], csend.at[par], crecv.at[par])
    c1 = summed(cbuf, par, 0, NDP) * sc_s[...]
    g1, v1 = rescale_first(c1)
    mine = core * 32
    e1 = v1 * sc_s[...]
    q1 = c1 * v1
    end_moments(0, [placed(p, mine + 16 * h) for p in (g1, e1, q1) for h in range(2)])
    ring_end(5)
    ring_end(6)
    wait(mbuf.at[0, 0:2 * NZ - 1], msend.at[0], mrecv.at[0])

    def over_blocks(par, cloud, first):
        rows = mbuf[par, cloud * NZ, first:first + 2]
        for b in range(1, NZ):
            rows = rows + mbuf[par, cloud * NZ + b, first:first + 2]
        return rows

    g_s[...] = over_blocks(0, core, 18)
    for i, cloud in enumerate((core, twin)):
        veff_s[i] = over_blocks(0, cloud, 20)
        qs_s[i] = over_blocks(0, cloud, 22)
    scales = [jnp.where(core == c, sc_s[...], pltpu.roll(sc_s[...], 32, 1)) for c in (0, 1)]
    for i in range(2):
        first = jnp.sum(jnp.where(lane == 0, scales[i], 0.0), axis=1, keepdims=True)
        a1_s[i:i + 1, :] = jnp.broadcast_to(first, (1, 128))

    def u_of_rows():
        for s in range(2):
            def body(b, accs):
                accs = list(accs)
                for j in range(4):
                    v = vb_s[j // 2, b, 8 * (j % 2):8 * (j % 2) + 8]
                    for t in range(tiles):
                        accs[t] = accs[t] + k_s[b, s, 8 * j:8 * j + 8, tile(t)] * v
                return tuple(accs)

            accs = lax.fori_loop(0, NZ, body, tuple(jnp.zeros((8, 128), f32) for _ in range(tiles)), unroll=True)
            for t in range(tiles):
                u_s[s, t:t + 1, :] = a_s[s, t:t + 1, :] / jnp.sum(accs[t], axis=0, keepdims=True)

    def start_columns(par):
        us = [[jnp.broadcast_to(u_s[s, t:t + 1, :], (8, 128)) for t in range(tiles)] for s in range(2)]

        def body(b, carry):
            for j in range(4):
                acc = [k_s[b, s, 8 * j:8 * j + 8, tile(t)] * us[s][t] for s in range(2) for t in range(tiles)]
                while len(acc) > 1:
                    acc = [p + q for p, q in zip(acc[::2], acc[1::2])]
                c_s[j // 2, b, 8 * (j % 2):8 * (j % 2) + 8] = acc[0]
            return carry

        lax.fori_loop(0, NZ, body, 0, unroll=True)
        slot = dbuf.at[par, core * (NDP // 2) + chip]
        slot[...] = jnp.concatenate([gather_rows(c_s[h].reshape(128, 128)) for h in range(2)], axis=0)
        send(slot, [dp_target(o) for o in DP_OFFSETS], dsend.at[par], drecv.at[par])

    def end_columns(par):
        wait(dbuf.at[par, 0:NDP - 1], dsend.at[par], drecv.at[par])
        c = [summed(dbuf, par, cloud * (NDP // 2), NDP // 2) * a1_s[i:i + 1] for i, cloud in enumerate((core, twin))]
        g = cube_root(k3_s[...] * ((v_s[0] * c[0]) * (v_s[1] * c[1])))
        for i in range(2):
            v_s[i] = g / c[i]
        return c, g

    def plain_step(step):
        par = lax.rem(step, 2)
        start_columns(par)
        end_columns(par)
        spread_all(vb_s, v_s[0])
        u_of_rows()

    def mirror(outer, carry):
        mpar = lax.rem(outer, 2)
        g = g_s[...]
        sq = [over_blocks(mpar, cloud, 16) * veff_s[i] for i, cloud in enumerate((core, twin))]
        cross = sq[0] * qs_s[1] + sq[1] * qs_s[0]
        prod = jnp.concatenate([mbuf[mpar, b, 0:16] * mbuf[mpar, NZ + b, 0:16] for b in range(NZ)], axis=0).T
        dots = jnp.concatenate([jnp.sum(prod[64 * h:64 * h + 64], axis=0, keepdims=True) for h in range(2)], axis=0)
        gg = -(cross - 2.0 * dots * (veff_s[0] * veff_s[1])) / (g * g)
        hh = sq[1] / g

        def mean(p):
            return jnp.sum(jnp.sum(p, axis=1, keepdims=True), axis=0, keepdims=True) / RANK

        k3_s[...] = g * jnp.exp(-STEP * (gg - mean(gg)))
        spread_all(fb_s, veff_s[1] * (2.0 * STEP * LOG2E) / g)
        spread_all(sb_s, (hh - mean(hh)) * (-STEP * LOG2E))
        spread_all(vb_s, veff_s[0])
        for b in range(NZ):
            m = mbuf[mpar, twin * NZ + b, 0:16]
            turned = pltpu.roll(m, 64, 1)
            for h, pair_of in ((0, jnp.where(lane < 64, m, turned)), (1, jnp.where(lane < 64, turned, m))):
                high, low = split(pair_of * fb_s[h, b])
                w4_s[32 * b + 16 * h:32 * b + 16 * h + 16, 0:128] = high
                w4_s[32 * b + 16 * h:32 * b + 16 * h + 16, 128:256] = low
        for s in range(2):
            for t in range(tiles // 2):
                cols = slice(t * 256, (t + 1) * 256)
                f = jnp.dot(w4_s[...], x4_s[s, :, cols], preferred_element_type=f32)
                ua = jnp.concatenate(
                    [jnp.broadcast_to(u_s[s, 2 * t + i:2 * t + i + 1, :], (16, 128)) for i in range(2)], axis=1
                )
                acc = jnp.zeros((8, 256), f32)
                for b in range(NZ):
                    for h in range(2):
                        rows = slice(16 * h, 16 * h + 16)
                        sh = sb_s[h, b]
                        q = vb_s[h, b]
                        e = jnp.exp2(f[32 * b + 16 * h:32 * b + 16 * h + 16] + jnp.concatenate([sh, sh], axis=1))
                        new = k_s[b, s, rows, cols] * ua * jnp.concatenate([q, q], axis=1) * e
                        k_s[b, s, rows, cols] = new
                        acc = acc + (new[0:8] + new[8:16])
                total = jnp.sum(acc, axis=0, keepdims=True)
                for i in range(2):
                    r = 2 * t + i
                    u_s[s, r:r + 1, :] = a_s[s, r:r + 1, :] / total[:, 128 * i:128 * i + 128]

        v_s[...] = jnp.ones((2, 2, 128), f32)

        @pl.when(outer == MIRROR - 1)
        def _():
            pair(4).start()

        base = outer * INNER

        def body(t, inner):
            plain_step(base + t)
            return inner

        lax.fori_loop(0, INNER - 1, body, 0)
        par = lax.rem(base + (INNER - 1), 2)
        npar = lax.rem(outer + 1, 2)

        @pl.when(outer < MIRROR - 1)
        def _():
            start_moments()

        @pl.when(outer == MIRROR - 1)
        def _():
            pair(5).start()

        start_columns(par)

        @pl.when(outer < MIRROR - 1)
        def _():
            middle_moments()

        @pl.when(outer == MIRROR - 1)
        def _():
            for t in range(tiles):
                ku_s[core, :, tile(t)] = k_s[z, core, :, tile(t)] * jnp.broadcast_to(u_s[core, t:t + 1, :], (32, 128))
            end_pair(4)
            end_pair(5)
            for t in range(tiles):
                ku_s[twin, :, tile(t)] = o_s[:, tile(t)] * jnp.broadcast_to(ou_s[t:t + 1, :], (32, 128))
            scaled().start()

        c, g = end_columns(par)
        g_s[...] = g
        for i in range(2):
            veff_s[i] = v_s[i] * a1_s[i:i + 1]
            qs_s[i] = c[i] * v_s[i]

        @pl.when(outer < MIRROR - 1)
        def _():
            end_moments(npar, ())
            wait(mbuf.at[npar, 0:2 * NZ - 1, 0:18], msend.at[npar], mrecv.at[npar])

        return carry

    lax.fori_loop(0, MIRROR, mirror, 0)
    for i, cloud in ((0, core), (1, twin)):
        spread_all((vb_s, fb_s)[i], veff_s[i] * RANK)
        for h in range(2):
            vo_ref[cloud, 16 * h:16 * h + 16] = (vb_s, fb_s)[i][h, z]
    own = [
        pltpu.roll(jnp.broadcast_to(g_s[h:h + 1], (8, 128)), lax.rem(128 + 16 * h - z * 16, 128), 1)[0:1] for h in range(2)
    ]
    wo_ref[...] = jnp.where(lane < 16, own[0], own[1]) * (RANK / total_count)
    scaled().wait()


def finish(ku_ref, vo_ref, w_ref, lo_ref, ro_ref, wo_ref):
    for side, ref in ((0, lo_ref), (1, ro_ref)):
        for t in range(ref.shape[1] // 128):
            cols = slice(t * 128, (t + 1) * 128)
            ref[:, cols] = ku_ref[side, :, cols] * vo_ref[side]
    wo_ref[...] = w_ref[:, 0:wo_ref.shape[1]]


def shards(cloud_x, cloud_y, mass_x, mass_y, left_start, right_start, weight_start):
    ranks, points = left_start.shape
    total_count = float(points * lax.axis_size("dp"))
    tiles = points // 128
    f32 = jnp.float32
    bf16 = jnp.bfloat16
    dma = pltpu.SemaphoreType.DMA
    vmem = pl.BlockSpec(memory_space=pltpu.VMEM)
    scaled, scales, weights = pl.pallas_call(
        functools.partial(kernel, total_count),
        name="sinkhorn",
        out_shape=(
            jax.ShapeDtypeStruct((2, ranks, points), f32),
            jax.ShapeDtypeStruct((2, ranks, 128), f32),
            jax.ShapeDtypeStruct((1, 128), f32),
        ),
        in_specs=[pl.BlockSpec(memory_space=pl.ANY)] * 7,
        out_specs=[pl.BlockSpec(memory_space=pl.ANY), vmem, vmem],
        scratch_shapes=[
            pltpu.VMEM((1, ranks), f32),
            pltpu.VMEM((2, ranks, points), f32),
            pltpu.VMEM((2, 64, points), f32),
            pltpu.VMEM((2, tiles, 128), f32),
            pltpu.VMEM((NZ, 2, ranks, points), f32),
            pltpu.VMEM((2, 64, points), f32),
            pltpu.VMEM((2, 256, points), bf16),
            pltpu.VMEM((256, 256), bf16),
            pltpu.VMEM((2, tiles, 128), f32),
            pltpu.VMEM((2 * tiles, 128), f32),
            pltpu.VMEM((2, tiles, 128), f32),
            pltpu.VMEM((2, tiles, 128), f32),
            pltpu.VMEM((2, tiles, 128), f32),
            pltpu.VMEM((2, 64, points), bf16),
            pltpu.VMEM((2, NZ, 16, 128), f32),
            pltpu.VMEM((64, 128), f32),
            pltpu.VMEM((2, NZ, 16, 128), f32),
            pltpu.VMEM((2, NZ, 16, 128), f32),
            pltpu.VMEM((2, NZ, 16, 128), f32),
            pltpu.VMEM((ranks, points), f32),
            pltpu.VMEM((tiles, 128), f32),
            pltpu.VMEM((2, ranks, points), f32),
            pltpu.VMEM((1, 128), f32),
            pltpu.VMEM((1, 128), f32),
            pltpu.VMEM((1, 128), f32),
            pltpu.VMEM((2, 2, 128), f32),
            pltpu.VMEM((2, 128), f32),
            pltpu.VMEM((2, 128), f32),
            pltpu.VMEM((2, 2, 128), f32),
            pltpu.VMEM((2, 2, 128), f32),
            pltpu.VMEM((2, NZ, 2 * tiles, 128), f32),
            pltpu.VMEM((2, NDP, 1, 128), f32),
            pltpu.VMEM((2, NDP, 2, 128), f32),
            pltpu.VMEM((NX, 18, 128), f32),
            pltpu.VMEM((NY, 18, 128), f32),
            pltpu.VMEM((2, 2 * NZ, 24, 128), f32),
            dma((2,)), dma((2,)), dma((2,)), dma((2,)), dma((2,)), dma((2,)),
            dma, dma, dma, dma, dma((2,)), dma((2,)),
            dma((NZ - 1, 2)), dma((NZ - 1, 2)), dma((6,)), dma((6,)), dma((8,)),
        ],
        compiler_params=pltpu.CompilerParams(collective_id=0, has_side_effects=True),
    )(
        cloud_x, cloud_y, mass_x.reshape(tiles, 128), mass_y.reshape(tiles, 128),
        left_start, right_start, weight_start[None],
    )
    left, right, weights = pl.pallas_call(
        finish,
        name="finish",
        out_shape=(
            jax.ShapeDtypeStruct((ranks, points), f32),
            jax.ShapeDtypeStruct((ranks, points), f32),
            jax.ShapeDtypeStruct((1, ranks), f32),
        ),
        in_specs=[vmem] * 3,
        out_specs=[vmem] * 3,
    )(scaled, scales, weights)
    return left, right, weights.reshape(ranks)


def solution(mesh):
    in_specs = (
        P(None, "dp"),
        P(None, "dp"),
        P("dp"),
        P("dp"),
        P("rank", "dp"),
        P("rank", "dp"),
        P("rank"),
    )
    out_specs = (P("rank", "dp"), P("rank", "dp"), P("rank"))
    return jax.shard_map(shards, mesh=mesh, in_specs=in_specs, out_specs=out_specs, check_vma=False)
```
